256 devices in a mesh: grp: 2 (over y), row: 128 (over x, z, core).
Axes of the slice: x: 4, y: 2, z: 16, core: 2. Of those that a mesh axis runs over, the one named last changes fastest.
The devices are a block of a 4x16x16 slice.
Arguments:
- diag_blocks: float32 [65536, 512], P('row'), may hold values from -0.6 to 2.6
- lower_coupling: float32 [65536, 64], P('row'), may hold values from -0.3125 to 0.3125
- upper_coupling: float32 [65536, 64], P('row'), may hold values from -0.3125 to 0.3125
- right_sides: float32 [65536, 1024], P('row', 'grp'), parts along dimension 1, may hold values from -108 to 108
Outputs:
- solution: float32 [65536, 1024], P('row', 'grp'), parts along dimension 1
- res_norms: float32 [8, 1024], P(None, 'grp'), parts along dimension 1
The draws below stay inside these ranges and needn't reach their ends.
There are 2 independent parts, one for each index of `grp`. The reference program is written for one: setup_inputs(seed, part) draws one part's arguments, and reference() takes and returns one part's arrays. A program takes and returns all parts, laid end to end along the dimension named above; an argument that names none is the same for every part. Nothing has to cross between parts.
All inputs are finite; a program needn't handle non-finite values.
Results may differ from the reference program's by a relative error of at most 0.0001.
Values sent between devices are 32-bit elements; how exact they have to be, the bound alone decides.
A program may use at most 64 MiB of HBM per device.

```python
import math
import jax
import jax.numpy as jnp
from jax import lax

B = 512
W = 64
C = 512
SWEEPS = 8
N = 65536
N_ROW = 128


def draw_diag_blocks(key, part):
    first, second = jax.random.split(jax.random.fold_in(key, 31), 2)
    noise = jnp.clip(jax.random.normal(first, (N, B), jnp.float32), -4.0, 4.0)
    noise = noise * (0.8 / math.sqrt(B))
    pivots = jax.random.uniform(second, (N, 1), jnp.float32, 1.0, 2.0)
    local_rows = (jnp.arange(N, dtype=jnp.int32) % B)[:, None]
    columns = jnp.arange(B, dtype=jnp.int32)[None, :]
    marker = (local_rows == columns).astype(jnp.float32)
    return (noise + marker * pivots).astype(jnp.float32)


def draw_right_sides(key, part):
    first, second, third = jax.random.split(jax.random.fold_in(key, 47), 3)
    base = jnp.clip(jax.random.normal(first, (N, C), jnp.float32), -4.0, 4.0)
    trend = jnp.exp(math.log(3.0) * jnp.arange(N, dtype=jnp.float32) / N)[:, None]
    row_scale = jnp.exp(jax.random.uniform(second, (N, 1), jnp.float32, math.log(0.3), math.log(3.0)))
    col_scale = jnp.exp(jax.random.uniform(third, (1, C), jnp.float32, math.log(0.3), math.log(3.0)))
    return (base * trend * row_scale * col_scale).astype(jnp.float32)


def block_levels(key, shape, shards, least, largest):
    gain = 1.0
    for position, parts in shards:
        draws = jax.random.uniform(jax.random.fold_in(jax.random.fold_in(key, 6), position), (parts,), jnp.float32, least / len(shards), largest / len(shards))
        gain = gain * jnp.repeat(jnp.exp(draws), shape[position] // parts).reshape((-1,) + (1,) * (len(shape) - 1 - position))
    return gain


def bell_draw(rng, extent, spread, most, shards=(), held_as=jnp.bfloat16):
    drawn = jax.random.normal(rng, extent, jnp.float32) * spread
    if len(shards) > 0:
        drawn = block_levels(rng, extent, shards, -0.22, 0.18) * drawn
    return jnp.clip(drawn, min=-most, max=most).astype(held_as)


def setup_inputs(seed: int = 0, part: int = 0) -> dict:
    seeds = jax.random.split(jax.random.key(seed), 5)
    part_keys = jax.random.split(jax.random.fold_in(seeds[4], part), 5)
    diag_blocks = draw_diag_blocks(jax.random.fold_in(seeds[4], 71), part)
    lower_coupling = bell_draw(seeds[1], (N, W), (6 * W) ** -0.5, 0.3125, ((0, 128),), jnp.float32)
    upper_coupling = bell_draw(seeds[2], (N, W), (6 * W) ** -0.5, 0.3125, ((0, 128),), jnp.float32)
    right_sides = draw_right_sides(jax.random.fold_in(jax.random.fold_in(seeds[4], part), 71), part)
    return dict(diag_blocks=diag_blocks, lower_coupling=lower_coupling, upper_coupling=upper_coupling, right_sides=right_sides)


def reference(diag_blocks, lower_coupling, upper_coupling, right_sides):
    blocks = diag_blocks.reshape(N_ROW, B, B)
    lower_blocks = lower_coupling.reshape(N_ROW, B, W)
    upper_blocks = upper_coupling.reshape(N_ROW, B, W)
    sources = right_sides.reshape(N_ROW, B, C)
    pivots = jnp.diagonal(blocks, axis1=1, axis2=2)[:, :, None]
    solution = jnp.zeros((N_ROW, B, C), jnp.float32)
    norm_list = []
    for sweep_index in range(SWEEPS):
        before_rims = jnp.concatenate([jnp.zeros((1, W, C), jnp.float32), solution[:-1, B - W:]], 0)
        after_rims = jnp.concatenate([solution[1:, :W], jnp.zeros((1, W, C), jnp.float32)], 0)
        images = jnp.einsum('kij,kjc->kic', blocks, solution, precision=lax.Precision.HIGHEST)
        images = images + jnp.einsum('kiw,kwc->kic', lower_blocks, before_rims, precision=lax.Precision.HIGHEST)
        images = images + jnp.einsum('kiw,kwc->kic', upper_blocks, after_rims, precision=lax.Precision.HIGHEST)
        residual = sources - images
        norm_list.append(jnp.sqrt(lax.optimization_barrier(jnp.sum(residual * residual, axis=(0, 1)))))
        solution = solution + residual / pivots
    return (solution.reshape(N_ROW * B, C), jnp.stack(norm_list))
```

```python
import functools

import jax
import jax.numpy as jnp
from jax import lax
from jax.experimental import pallas as pl
from jax.experimental.pallas import tpu as pltpu
from jax.sharding import PartitionSpec as P

MESH = pl.DeviceIdType.MESH
SWEEPS = 8
DEPTH = 16
CORES = 2
CHUNKS = 2
F32 = jnp.float32
BF16 = jnp.bfloat16


def split(value):
    hi = value.astype(BF16)
    return hi, (value - hi.astype(F32)).astype(BF16)


def dot(left, right):
    return jnp.dot(left, right, preferred_element_type=F32)


def kernel(
    n, diag_hbm, lower_hbm, upper_hbm, rhs_hbm, x_acc, norms_ref,
    diag, lower, upper, rhs, recip, pivot, mats, edges, gmat_in, gmat_out, parts, ends_in, ends_out, inner_z,
    add_in, add_out, send_in, recv_in, send_out, recv_out, gsend_in, grecv_in, gsend_out, grecv_out,
    sums, early_plane, early_line, early_rows, late_plane, late_line,
    load_sem, si_sem, ri_sem, so_sem, ro_sem, g_sem,
    ap_send, ap_recv, bp_send, bp_recv, cp_send, cp_recv, al_send, al_recv, bl_send, bl_recv, know_a, know_b,
):
    width, size = lower_hbm.shape
    cols = rhs_hbm.shape[1]
    chunk = cols // CHUNKS
    last = SWEEPS - 1
    me = lax.axis_index("row")
    core = lax.rem(me, CORES)
    chip = lax.div(me, CORES)
    depth = lax.rem(chip, DEPTH)
    plane = lax.div(chip, DEPTH)
    planes = n // (CORES * DEPTH)
    members = planes * CORES
    place = plane * CORES + core
    near = me + 1 - 2 * core
    far = me - 1 + 2 * core
    has_far = jnp.logical_and(far >= 0, far < n)
    far_rows = pl.multiple_of(core * (size - width), width)
    near_rows = pl.multiple_of((1 - core) * (size - width), width)

    def at_place(other):
        return (lax.div(other, CORES) * DEPTH + depth) * CORES + lax.rem(other, CORES)

    def at_depth(other):
        return (plane * DEPTH + other) * CORES + core

    def signal(sem, target):
        pl.semaphore_signal(sem, inc=1, device_id={"row": target}, device_id_type=MESH)

    def remote(src, dst, send_sem, recv_sem, target):
        return pltpu.make_async_remote_copy(
            src_ref=src, dst_ref=dst, send_sem=send_sem, recv_sem=recv_sem,
            device_id={"row": target}, device_id_type=MESH,
        )

    slab = size // 4
    loads = []

    def load(src, dst):
        copy = pltpu.make_async_copy(src, dst, load_sem.at[len(loads)])
        copy.start()
        loads.append(copy)
        return copy

    diag_loads, rhs_loads = {}, {}
    for i in (0, 3):
        diag_loads[i] = load(diag_hbm.at[pl.ds(i * slab, slab)], diag.at[pl.ds(i * slab, slab)])
        rhs_loads[i] = load(rhs_hbm.at[pl.ds(i * slab, slab)], rhs.at[pl.ds(i * slab, slab)])
    lower_load = load(lower_hbm, lower)
    upper_load = load(upper_hbm, upper)
    for i in (1, 2):
        diag_loads[i] = load(diag_hbm.at[pl.ds(i * slab, slab)], diag.at[pl.ds(i * slab, slab)])
        rhs_loads[i] = load(rhs_hbm.at[pl.ds(i * slab, slab)], rhs.at[pl.ds(i * slab, slab)])

    barrier = pltpu.get_barrier_semaphore()
    for offset in range(1, members):
        signal(barrier, at_place(lax.rem(place + offset, members)))
    for offset in (1, 2, DEPTH - 2, DEPTH - 1):
        signal(barrier, at_depth(lax.rem(depth + offset, DEPTH)))

    @pl.when(has_far)
    def _():
        signal(barrier, far)

    @pl.when(jnp.logical_not(has_far))
    def _():
        recv_out[...] = jnp.zeros_like(recv_out)
        grecv_out[...] = jnp.zeros_like(grecv_out)

    add_in[...] = jnp.zeros_like(add_in)
    add_out[...] = jnp.zeros_like(add_out)

    mask = lax.broadcasted_iota(jnp.int32, (slab, slab), 0) == lax.broadcasted_iota(jnp.int32, (slab, slab), 1)

    def pivots(i):
        rows = pl.ds(i * slab, slab)
        block = diag[rows, pl.ds(i * slab, slab)]
        values = jnp.sum(jnp.where(mask, block, 0.0), axis=1, keepdims=True)
        pivot[rows, :] = jnp.broadcast_to(values, (slab, slab))
        first = 1.0 / values
        recip[rows, :] = jnp.broadcast_to(first + first * (1.0 - values * first), (slab, slab))

    def scale(block, rows):
        factor = recip[rows, :]
        return jnp.concatenate([block[:, j : j + slab] * factor for j in range(0, block.shape[1], slab)], axis=1)

    for i in (0, 3):
        diag_loads[i].wait()
        pivots(i)
    for i in (0, 3):
        rhs_loads[i].wait()
    for ch in range(CHUNKS):
        span = pl.ds(ch * chunk, chunk)
        near_slice, far_slice = pl.ds(near_rows, width), pl.ds(far_rows, width)
        send_out[0, ch] = scale(rhs[far_slice, span], far_slice)
        send_in[0, ch] = scale(rhs[near_slice, span], near_slice)

    @pl.when(has_far)
    def _():
        pl.semaphore_wait(barrier, members + 4)

    @pl.when(jnp.logical_not(has_far))
    def _():
        pl.semaphore_wait(barrier, members + 3)

    def near_copy(s, ch):
        return remote(send_in.at[s, ch], recv_in.at[s, ch], si_sem.at[s, ch], ri_sem.at[s, ch], near)

    def far_copy(s, ch):
        return remote(send_out.at[s, ch], recv_out.at[s, ch], so_sem.at[s, ch], ro_sem.at[s, ch], far)

    def g_copy_near():
        return remote(gsend_in, grecv_in, g_sem.at[0], g_sem.at[1], near)

    def g_copy_far():
        return remote(gsend_out, grecv_out, g_sem.at[2], g_sem.at[3], far)

    def if_far(action):
        @pl.when(has_far)
        def _():
            action()

    for ch in range(CHUNKS):
        if_far(lambda ch=ch: far_copy(0, ch).start())
        near_copy(0, ch).start()
    signal(know_a, at_depth(lax.rem(depth + 2, DEPTH)))
    signal(know_a, at_depth(lax.rem(depth + DEPTH - 2, DEPTH)))

    for i in (1, 2):
        diag_loads[i].wait()
        pivots(i)
    lower_load.wait()
    upper_load.wait()
    for i in range(4):
        rows = pl.ds(i * slab, slab)
        low, up = lower[:, rows].T, upper[:, rows].T
        to_near = jnp.where(core == 0, up, low)
        to_far = jnp.where(has_far, jnp.where(core == 0, low, up), 0.0)
        for position, block in enumerate((to_near, to_far)):
            twice = jnp.concatenate([block, block], axis=1) * (-recip[rows, :])
            hi, lo = split(twice)
            edges[rows, pl.ds(position * 2 * slab, slab)] = hi
            edges[rows, pl.ds(position * 2 * slab + slab, slab)] = lo

    def rejoin(rows, position):
        hi = edges[rows, pl.ds(position * 2 * slab, slab)].astype(F32)
        return hi + edges[rows, pl.ds(position * 2 * slab + slab, slab)].astype(F32)

    gsend_in[...] = rejoin(pl.ds(near_rows, width), 0)
    gsend_out[...] = rejoin(pl.ds(far_rows, width), 1)
    if_far(lambda: g_copy_far().start())
    g_copy_near().start()

    for i in range(4):
        rows = pl.ds(i * slab, slab)
        factor = -recip[rows, :]
        for j in range(4):
            block = diag[rows, pl.ds(j * slab, slab)]
            if i == j:
                block = jnp.where(mask, 0.0, block)
            hi, lo = split(block * factor)
            mats[rows, pl.ds(j * slab, slab)] = hi
            mats[rows, pl.ds(size + j * slab, slab)] = hi
            mats[rows, pl.ds(2 * size + j * slab, slab)] = lo

    for i in (1, 2):
        rhs_loads[i].wait()

    tile = 64

    def rows_sum(total):
        return jnp.sum(total, axis=0, keepdims=True)

    def keep(ch, r, value):
        hi, lo = split(value)
        parts[ch, pl.ds(r, tile), :] = hi
        parts[ch, pl.ds(size + r, tile), :] = lo

    def begin(ch):
        span = pl.ds(ch * chunk, chunk)
        total = jnp.zeros((8, chunk), F32)
        for r in range(0, size, tile):
            rows = pl.ds(r, tile)
            block = rhs[rows, span]
            total += jnp.sum((block * block).reshape(tile // 8, 8, chunk), axis=0)
            value = scale(block, rows)
            x_acc[rows, span] = value
            keep(ch, r, value)
        sums[0, :, span] = rows_sum(total)

    def advance(ch):
        low_high = parts[ch]
        inner_z[ch] = dot(mats[...], jnp.concatenate([low_high, low_high[:size]], axis=0))

    def echo(ch):
        for rows, gmat, add in ((near_rows, gmat_in, add_in), (far_rows, gmat_out, add_out)):
            hi = parts[ch, pl.ds(rows, width), :]
            lo = parts[ch, pl.ds(size + rows, width), :]
            add[ch] = dot(gmat[...], jnp.concatenate([hi, lo, hi, lo], axis=0))

    def take(ch, received, add, ends):
        hi, lo = split(received + add[ch])
        ends[ch] = jnp.concatenate([hi, lo, hi, lo], axis=0)

    def from_near(s, ch, send):
        near_copy(s, ch).wait_recv()
        take(ch, recv_in[s, ch], add_in, ends_in)
        if send:
            rows = pl.ds(far_rows, width)
            send_out[s + 1, ch] = inner_z[ch, rows, :] + dot(edges[rows, : 2 * slab], ends_in[ch])
            if_far(lambda: far_copy(s + 1, ch).start())

    def from_far(s, ch, send):
        if_far(lambda: far_copy(s, ch).wait_recv())
        take(ch, recv_out[s, ch], add_out, ends_out)
        if send:
            rows = pl.ds(near_rows, width)
            send_in[s + 1, ch] = inner_z[ch, rows, :] + dot(edges[rows, 2 * slab :], ends_out[ch])
            near_copy(s + 1, ch).start()

    def complete(s, ch, final):
        span = pl.ds(ch * chunk, chunk)
        inner_z[ch] += dot(edges[...], jnp.concatenate([ends_in[ch], ends_out[ch]], axis=0))
        total = jnp.zeros((8, chunk), F32)
        for r in range(0, size, tile):
            rows = pl.ds(r, tile)
            value = inner_z[ch, rows, :]
            x_acc[rows, span] += value
            if not final:
                keep(ch, r, value)
            factor = pivot[rows, :]
            residual = jnp.concatenate([value[:, j : j + slab] * factor for j in range(0, chunk, slab)], axis=1)
            total += jnp.sum((residual * residual).reshape(tile // 8, 8, chunk), axis=0)
        sums[s + 1, :, span] = rows_sum(total)

    for ch in range(CHUNKS):
        begin(ch)
        advance(ch)

    def sweep(s, carry):
        for ch in range(CHUNKS):
            from_near(s, ch, True)
        for ch in range(CHUNKS):
            from_far(s, ch, True)
            if ch == 0:

                if s == 0:
                    g_copy_near().wait_recv()
                    if_far(lambda: g_copy_far().wait_recv())
                    for source, target in ((grecv_in, gmat_in), (grecv_out, gmat_out)):
                        hi, lo = split(source[...])
                        target[:, :slab] = hi
                        target[:, slab:] = lo

            echo(ch)
            complete(s, ch, False)
            advance(ch)
        return carry

    for s in range(last - 1):
        sweep(s, 0)

    def spread(count, index, at, copy):
        for offset in range(1, count):
            copy(offset, lax.rem(index + offset, count))

    def early_a(offset, target_place):
        return remote(
            sums.at[target_place], early_plane.at[place], ap_send.at[offset], ap_recv.at[offset], at_place(target_place)
        )

    for offset in range(1, members):
        target_place = lax.rem(place + offset, members)

        @pl.when(target_place != last)
        def _(offset=offset, target_place=target_place):
            early_a(offset, target_place).start()

    pl.semaphore_wait(know_a, 2)
    signal(know_b, at_depth(lax.rem(depth + 4, DEPTH)))
    signal(know_b, at_depth(lax.rem(depth + DEPTH - 4, DEPTH)))

    for ch in range(CHUNKS):
        from_near(last - 1, ch, False)
    for ch in range(CHUNKS):
        from_far(last - 1, ch, False)
        complete(last - 1, ch, True)

    def late_a(offset):
        return remote(
            sums.at[last], late_plane.at[place], al_send.at[offset], al_recv.at[offset],
            at_place(lax.rem(place + offset, members)),
        )

    def line(buffer, send_sem, recv_sem, offset):
        return remote(
            buffer.at[depth], buffer.at[depth], send_sem.at[offset], recv_sem.at[offset],
            at_depth(lax.rem(depth + offset, DEPTH)),
        )

    def early_c(offset):
        return remote(
            early_rows.at[place], early_rows.at[place], cp_send.at[offset], cp_recv.at[offset],
            at_place(lax.rem(place + offset, members)),
        )

    def added(buffer, count):
        values = [buffer[i] for i in range(count)]
        while len(values) > 1:
            values = [values[i] + values[i + 1] for i in range(0, len(values), 2)]
        return values[0]

    for offset in range(1, members):
        late_a(offset).start()
    late_plane[place] = sums[last]
    pl.semaphore_wait(know_b, 2)

    @pl.when(place != last)
    def _():
        early_plane[place] = sums[place]
        for offset in range(1, members):
            early_a(offset, place).wait_recv()
        early_line[depth] = added(early_plane, members)
        for offset in range(1, DEPTH):
            line(early_line, bp_send, bp_recv, offset).start()

    for offset in range(1, members):
        late_a(offset).wait_recv()
    late_line[depth] = added(late_plane, members)
    for offset in range(1, DEPTH):
        line(late_line, bl_send, bl_recv, offset).start()

    @pl.when(place != last)
    def _():
        for offset in range(1, DEPTH):
            line(early_line, bp_send, bp_recv, offset).wait_recv()
        early_rows[place] = added(early_line, DEPTH)
        for offset in range(1, members):
            early_c(offset).start()

    for offset in range(1, DEPTH):
        line(late_line, bl_send, bl_recv, offset).wait_recv()
    norms_ref[last : last + 1, :] = jnp.sqrt(added(late_line, DEPTH))
    for offset in range(1, members):

        @pl.when(lax.rem(place + members - offset, members) != last)
        def _(offset=offset):
            early_c(offset).wait_recv()

    for i in range(last):
        norms_ref[i : i + 1, :] = jnp.sqrt(early_rows[i])

    for s in range(last):
        for ch in range(CHUNKS):
            near_copy(s, ch).wait_send()
            if_far(lambda s=s, ch=ch: far_copy(s, ch).wait_send())
    g_copy_near().wait_send()
    if_far(lambda: g_copy_far().wait_send())
    for offset in range(1, members):
        late_a(offset).wait_send()

        @pl.when(lax.rem(place + offset, members) != last)
        def _(offset=offset):
            early_a(offset, place).wait_send()

    for offset in range(1, DEPTH):
        line(late_line, bl_send, bl_recv, offset).wait_send()

    @pl.when(place != last)
    def _():
        for offset in range(1, DEPTH):
            line(early_line, bp_send, bp_recv, offset).wait_send()
        for offset in range(1, members):
            early_c(offset).wait_send()


def solution(mesh):
    n = mesh.shape["row"]
    members = n // DEPTH

    def step(diag_blocks, lower_coupling, upper_coupling, right_sides):
        size, width = lower_coupling.shape
        cols = right_sides.shape[1]
        chunk = cols // CHUNKS
        last = SWEEPS - 1
        dma = pltpu.SemaphoreType.DMA
        halo = pltpu.VMEM((last, CHUNKS, width, chunk), F32)
        square = pltpu.VMEM((width, 2 * width), F32)
        row = lambda count: pltpu.VMEM((count, 1, cols), F32)
        return pl.pallas_call(
            functools.partial(kernel, n),
            out_shape=(
                jax.ShapeDtypeStruct((size, cols), F32),
                jax.ShapeDtypeStruct((SWEEPS, cols), F32),
            ),
            in_specs=[pl.BlockSpec(memory_space=pltpu.HBM)] * 4,
            out_specs=(pl.BlockSpec(memory_space=pltpu.VMEM), pl.BlockSpec(memory_space=pltpu.VMEM)),
            scratch_shapes=[
                pltpu.VMEM((size, size), F32),
                pltpu.VMEM((width, size), F32),
                pltpu.VMEM((width, size), F32),
                pltpu.VMEM((size, cols), F32),
                pltpu.VMEM((size, size // 4), F32),
                pltpu.VMEM((size, size // 4), F32),
                pltpu.VMEM((size, 3 * size), BF16),
                pltpu.VMEM((size, 8 * width), BF16),
                pltpu.VMEM((width, 4 * width), BF16),
                pltpu.VMEM((width, 4 * width), BF16),
                pltpu.VMEM((CHUNKS, 2 * size, chunk), BF16),
                pltpu.VMEM((CHUNKS, 4 * width, chunk), BF16),
                pltpu.VMEM((CHUNKS, 4 * width, chunk), BF16),
                pltpu.VMEM((CHUNKS, size, chunk), F32),
                pltpu.VMEM((CHUNKS, width, chunk), F32),
                pltpu.VMEM((CHUNKS, width, chunk), F32),
                halo, halo, halo, halo,
                square, square, square, square,
                row(SWEEPS), row(members), row(DEPTH), row(members), row(members), row(DEPTH),
                dma((10,)),
                dma((last, CHUNKS)), dma((last, CHUNKS)), dma((last, CHUNKS)), dma((last, CHUNKS)), dma((4,)),
                dma((members,)), dma((members,)), dma((DEPTH,)), dma((DEPTH,)), dma((members,)), dma((members,)),
                dma((members,)), dma((members,)), dma((DEPTH,)), dma((DEPTH,)),
                pltpu.SemaphoreType.REGULAR, pltpu.SemaphoreType.REGULAR,
            ],
            compiler_params=pltpu.CompilerParams(
                collective_id=0, has_side_effects=True, vmem_limit_bytes=40 * 1024 * 1024
            ),
        )(*(
            pltpu.with_memory_space_constraint(array, pltpu.HBM)
            for array in (diag_blocks, lower_coupling.T, upper_coupling.T, right_sides)
        ))

    return jax.shard_map(
        step,
        mesh=mesh,
        in_specs=(P("row", None), P("row", None), P("row", None), P("row", "grp")),
        out_specs=(P("row", "grp"), P(None, "grp")),
        check_vma=False,
    )
```

```python
import functools

import jax
import jax.numpy as jnp
from jax import lax
from jax.experimental import pallas as pl
from jax.experimental.pallas import tpu as pltpu
from jax.sharding import PartitionSpec as P

MESH = pl.DeviceIdType.MESH
SWEEPS = 8
DEPTH = 16
CORES = 2
CHUNKS = 2
F32 = jnp.float32
BF16 = jnp.bfloat16


def split(value):
    hi = value.astype(BF16)
    return hi, (value - hi.astype(F32)).astype(BF16)


def dot(left, right):
    return jnp.dot(left, right, preferred_element_type=F32)


def kernel(
    n, diag_hbm, lower_hbm, upper_hbm, rhs_hbm, x_acc, norms_ref,
    diag, lower, upper, rhs, recip, pivot, mats, edges, gmat_in, gmat_out, parts, ends_in, ends_out, inner_z,
    add_in, add_out, send_in, recv_in, send_out, recv_out, gsend_in, grecv_in, gsend_out, grecv_out,
    sums, early_plane, early_line, early_rows, late_plane, late_line,
    load_sem, si_sem, ri_sem, so_sem, ro_sem, g_sem,
    ap_send, ap_recv, bp_send, bp_recv, cp_send, cp_recv, al_send, al_recv, bl_send, bl_recv, know_a, know_b,
):
    width, size = lower_hbm.shape
    cols = rhs_hbm.shape[1]
    chunk = cols // CHUNKS
    last = SWEEPS - 1
    early = SWEEPS - 2
    me = lax.axis_index("row")
    core = lax.rem(me, CORES)
    chip = lax.div(me, CORES)
    depth = lax.rem(chip, DEPTH)
    plane = lax.div(chip, DEPTH)
    planes = n // (CORES * DEPTH)
    members = planes * CORES
    place = plane * CORES + core
    near = me + 1 - 2 * core
    far = me - 1 + 2 * core
    has_far = jnp.logical_and(far >= 0, far < n)
    far_rows = pl.multiple_of(core * (size - width), width)
    near_rows = pl.multiple_of((1 - core) * (size - width), width)

    def at_place(other):
        return (lax.div(other, CORES) * DEPTH + depth) * CORES + lax.rem(other, CORES)

    def at_depth(other):
        return (plane * DEPTH + other) * CORES + core

    def signal(sem, target):
        pl.semaphore_signal(sem, inc=1, device_id={"row": target}, device_id_type=MESH)

    def remote(src, dst, send_sem, recv_sem, target):
        return pltpu.make_async_remote_copy(
            src_ref=src, dst_ref=dst, send_sem=send_sem, recv_sem=recv_sem,
            device_id={"row": target}, device_id_type=MESH,
        )

    slab = size // 4
    loads = []

    def load(src, dst):
        copy = pltpu.make_async_copy(src, dst, load_sem.at[len(loads)])
        copy.start()
        loads.append(copy)
        return copy

    diag_loads, rhs_loads = {}, {}
    for i in (0, 3):
        diag_loads[i] = load(diag_hbm.at[pl.ds(i * slab, slab)], diag.at[pl.ds(i * slab, slab)])
        rhs_loads[i] = load(rhs_hbm.at[pl.ds(i * slab, slab)], rhs.at[pl.ds(i * slab, slab)])
    lower_load = load(lower_hbm, lower)
    upper_load = load(upper_hbm, upper)
    for i in (1, 2):
        diag_loads[i] = load(diag_hbm.at[pl.ds(i * slab, slab)], diag.at[pl.ds(i * slab, slab)])
        rhs_loads[i] = load(rhs_hbm.at[pl.ds(i * slab, slab)], rhs.at[pl.ds(i * slab, slab)])

    barrier = pltpu.get_barrier_semaphore()
    for offset in range(1, members):
        signal(barrier, at_place(lax.rem(place + offset, members)))
    for offset in (1, 2, DEPTH - 2, DEPTH - 1):
        signal(barrier, at_depth(lax.rem(depth + offset, DEPTH)))

    @pl.when(has_far)
    def _():
        signal(barrier, far)

    @pl.when(jnp.logical_not(has_far))
    def _():
        recv_out[...] = jnp.zeros_like(recv_out)
        grecv_out[...] = jnp.zeros_like(grecv_out)

    add_in[...] = jnp.zeros_like(add_in)
    add_out[...] = jnp.zeros_like(add_out)

    mask = lax.broadcasted_iota(jnp.int32, (slab, slab), 0) == lax.broadcasted_iota(jnp.int32, (slab, slab), 1)

    def pivots(i):
        rows = pl.ds(i * slab, slab)
        block = diag[rows, pl.ds(i * slab, slab)]
        values = jnp.sum(jnp.where(mask, block, 0.0), axis=1, keepdims=True)
        pivot[rows, :] = jnp.broadcast_to(values, (slab, slab))
        first = 1.0 / values
        recip[rows, :] = jnp.broadcast_to(first + first * (1.0 - values * first), (slab, slab))

    def scale(block, rows):
        factor = recip[rows, :]
        return jnp.concatenate([block[:, j : j + slab] * factor for j in range(0, block.shape[1], slab)], axis=1)

    for i in (0, 3):
        diag_loads[i].wait()
        pivots(i)
    for i in (0, 3):
        rhs_loads[i].wait()
    for ch in range(CHUNKS):
        span = pl.ds(ch * chunk, chunk)
        near_slice, far_slice = pl.ds(near_rows, width), pl.ds(far_rows, width)
        send_out[0, ch] = scale(rhs[far_slice, span], far_slice)
        send_in[0, ch] = scale(rhs[near_slice, span], near_slice)

    @pl.when(has_far)
    def _():
        pl.semaphore_wait(barrier, members + 4)

    @pl.when(jnp.logical_not(has_far))
    def _():
        pl.semaphore_wait(barrier, members + 3)

    def near_copy(s, ch):
        return remote(send_in.at[s, ch], recv_in.at[s, ch], si_sem.at[s, ch], ri_sem.at[s, ch], near)

    def far_copy(s, ch):
        return remote(send_out.at[s, ch], recv_out.at[s, ch], so_sem.at[s, ch], ro_sem.at[s, ch], far)

    def g_copy_near():
        return remote(gsend_in, grecv_in, g_sem.at[0], g_sem.at[1], near)

    def g_copy_far():
        return remote(gsend_out, grecv_out, g_sem.at[2], g_sem.at[3], far)

    def if_far(action):
        @pl.when(has_far)
        def _():
            action()

    for ch in range(CHUNKS):
        if_far(lambda ch=ch: far_copy(0, ch).start())
        near_copy(0, ch).start()
    signal(know_a, at_depth(lax.rem(depth + 2, DEPTH)))
    signal(know_a, at_depth(lax.rem(depth + DEPTH - 2, DEPTH)))

    for i in (1, 2):
        diag_loads[i].wait()
        pivots(i)
    lower_load.wait()
    upper_load.wait()
    for i in range(4):
        rows = pl.ds(i * slab, slab)
        low, up = lower[:, rows].T, upper[:, rows].T
        to_near = jnp.where(core == 0, up, low)
        to_far = jnp.where(has_far, jnp.where(core == 0, low, up), 0.0)
        for position, block in enumerate((to_near, to_far)):
            twice = jnp.concatenate([block, block], axis=1) * (-recip[rows, :])
            hi, lo = split(twice)
            edges[rows, pl.ds(position * 2 * slab, slab)] = hi
            edges[rows, pl.ds(position * 2 * slab + slab, slab)] = lo

    def rejoin(rows, position):
        hi = edges[rows, pl.ds(position * 2 * slab, slab)].astype(F32)
        return hi + edges[rows, pl.ds(position * 2 * slab + slab, slab)].astype(F32)

    gsend_in[...] = rejoin(pl.ds(near_rows, width), 0)
    gsend_out[...] = rejoin(pl.ds(far_rows, width), 1)
    if_far(lambda: g_copy_far().start())
    g_copy_near().start()

    for i in range(4):
        rows = pl.ds(i * slab, slab)
        factor = -recip[rows, :]
        for j in range(4):
            block = diag[rows, pl.ds(j * slab, slab)]
            if i == j:
                block = jnp.where(mask, 0.0, block)
            hi, lo = split(block * factor)
            mats[rows, pl.ds(j * slab, slab)] = hi
            mats[rows, pl.ds(size + j * slab, slab)] = hi
            mats[rows, pl.ds(2 * size + j * slab, slab)] = lo

    for i in (1, 2):
        rhs_loads[i].wait()

    tile = 64

    def rows_sum(total):
        return jnp.sum(total, axis=0, keepdims=True)

    def keep(ch, r, value):
        hi, lo = split(value)
        parts[ch, pl.ds(r, tile), :] = hi
        parts[ch, pl.ds(size + r, tile), :] = lo

    def begin(ch):
        span = pl.ds(ch * chunk, chunk)
        total = jnp.zeros((8, chunk), F32)
        for r in range(0, size, tile):
            rows = pl.ds(r, tile)
            block = rhs[rows, span]
            total += jnp.sum((block * block).reshape(tile // 8, 8, chunk), axis=0)
            value = scale(block, rows)
            x_acc[rows, span] = value
            keep(ch, r, value)
        sums[0, :, span] = rows_sum(total)

    def advance(ch):
        low_high = parts[ch]
        inner_z[ch] = dot(mats[...], jnp.concatenate([low_high, low_high[:size]], axis=0))

    def echo(ch):
        for rows, gmat, add in ((near_rows, gmat_in, add_in), (far_rows, gmat_out, add_out)):
            hi = parts[ch, pl.ds(rows, width), :]
            lo = parts[ch, pl.ds(size + rows, width), :]
            add[ch] = dot(gmat[...], jnp.concatenate([hi, lo, hi, lo], axis=0))

    def take(ch, received, add, ends):
        hi, lo = split(received + add[ch])
        ends[ch] = jnp.concatenate([hi, lo, hi, lo], axis=0)

    def from_near(s, ch, send):
        near_copy(s, ch).wait_recv()
        take(ch, recv_in[s, ch], add_in, ends_in)
        if send:
            rows = pl.ds(far_rows, width)
            send_out[s + 1, ch] = inner_z[ch, rows, :] + dot(edges[rows, : 2 * slab], ends_in[ch])
            if_far(lambda: far_copy(s + 1, ch).start())

    def from_far(s, ch, send):
        if_far(lambda: far_copy(s, ch).wait_recv())
        take(ch, recv_out[s, ch], add_out, ends_out)
        if send:
            rows = pl.ds(near_rows, width)
            send_in[s + 1, ch] = inner_z[ch, rows, :] + dot(edges[rows, 2 * slab :], ends_out[ch])
            near_copy(s + 1, ch).start()

    def complete(s, ch, final):
        span = pl.ds(ch * chunk, chunk)
        inner_z[ch] += dot(edges[...], jnp.concatenate([ends_in[ch], ends_out[ch]], axis=0))
        total = jnp.zeros((8, chunk), F32)
        for r in range(0, size, tile):
            rows = pl.ds(r, tile)
            value = inner_z[ch, rows, :]
            x_acc[rows, span] += value
            if not final:
                keep(ch, r, value)
            factor = pivot[rows, :]
            residual = jnp.concatenate([value[:, j : j + slab] * factor for j in range(0, chunk, slab)], axis=1)
            total += jnp.sum((residual * residual).reshape(tile // 8, 8, chunk), axis=0)
        sums[s + 1, :, span] = rows_sum(total)

    for ch in range(CHUNKS):
        begin(ch)
        advance(ch)

    def take_squares():
        g_copy_near().wait_recv()
        if_far(lambda: g_copy_far().wait_recv())
        for source, target in ((grecv_in, gmat_in), (grecv_out, gmat_out)):
            hi, lo = split(source[...])
            target[:, :slab] = hi
            target[:, slab:] = lo

    def sweep(s):
        for ch in range(CHUNKS):
            from_far(s, ch, True)
            if ch > 0:
                from_near(s + 1, ch - 1, s + 1 < last - 1)
            elif s == 0:
                take_squares()
            echo(ch)
            complete(s, ch, False)
            advance(ch)
        from_near(s + 1, CHUNKS - 1, s + 1 < last - 1)

    def early_a(offset, target_place):
        return remote(
            sums.at[target_place], early_plane.at[place], ap_send.at[offset], ap_recv.at[offset], at_place(target_place)
        )

    def line(buffer, send_sem, recv_sem, offset):
        return remote(
            buffer.at[depth], buffer.at[depth], send_sem.at[offset], recv_sem.at[offset],
            at_depth(lax.rem(depth + offset, DEPTH)),
        )

    def late_a(offset):
        return remote(
            sums.at[pl.ds(early, SWEEPS - early)], late_plane.at[place], al_send.at[offset], al_recv.at[offset],
            at_place(lax.rem(place + offset, members)),
        )

    def early_c(offset):
        return remote(
            early_rows.at[place], early_rows.at[place], cp_send.at[offset], cp_recv.at[offset],
            at_place(lax.rem(place + offset, members)),
        )

    def added(buffer, count):
        values = [buffer[i] for i in range(count)]
        while len(values) > 1:
            values = [values[i] + values[i + 1] for i in range(0, len(values), 2)]
        return values[0]

    for ch in range(CHUNKS):
        from_near(0, ch, True)
    for s in range(early - 1):
        sweep(s)

    for offset in range(1, members):
        target_place = lax.rem(place + offset, members)

        @pl.when(target_place < early)
        def _(offset=offset, target_place=target_place):
            early_a(offset, target_place).start()

    pl.semaphore_wait(know_a, 2)
    signal(know_b, at_depth(lax.rem(depth + 4, DEPTH)))
    signal(know_b, at_depth(lax.rem(depth + DEPTH - 4, DEPTH)))
    for s in range(early - 1, last - 1):
        sweep(s)
    pl.semaphore_wait(know_b, 2)

    @pl.when(place < early)
    def _():
        early_plane[place] = sums[place]
        for offset in range(1, members):
            early_a(offset, place).wait_recv()
        early_line[depth] = added(early_plane, members)
        for offset in range(1, DEPTH):
            line(early_line, bp_send, bp_recv, offset).start()

    for ch in range(CHUNKS):
        from_far(last - 1, ch, False)
        complete(last - 1, ch, True)

    for offset in range(1, members):
        late_a(offset).start()
    late_plane[place] = sums[early:]

    for s in range(last):
        for ch in range(CHUNKS):
            near_copy(s, ch).wait_send()
            if_far(lambda s=s, ch=ch: far_copy(s, ch).wait_send())
    g_copy_near().wait_send()
    if_far(lambda: g_copy_far().wait_send())
    for offset in range(1, members):

        @pl.when(lax.rem(place + offset, members) < early)
        def _(offset=offset):
            early_a(offset, place).wait_send()

    for offset in range(1, members):
        late_a(offset).wait_recv()
    late_line[depth] = added(late_plane, members)
    for offset in range(1, DEPTH):
        line(late_line, bl_send, bl_recv, offset).start()

    @pl.when(place < early)
    def _():
        for offset in range(1, DEPTH):
            line(early_line, bp_send, bp_recv, offset).wait_recv()
        early_rows[place] = added(early_line, DEPTH)
        for offset in range(1, members):
            early_c(offset).start()

    for offset in range(1, members):

        @pl.when(lax.rem(place + members - offset, members) < early)
        def _(offset=offset):
            early_c(offset).wait_recv()

    for i in range(early):
        norms_ref[i : i + 1, :] = jnp.sqrt(early_rows[i])
    for offset in range(1, members):
        late_a(offset).wait_send()

    @pl.when(place < early)
    def _():
        for offset in range(1, DEPTH):
            line(early_line, bp_send, bp_recv, offset).wait_send()
        for offset in range(1, members):
            early_c(offset).wait_send()

    for offset in range(1, DEPTH):
        line(late_line, bl_send, bl_recv, offset).wait_send()
    for offset in range(1, DEPTH):
        line(late_line, bl_send, bl_recv, offset).wait_recv()
    total = added(late_line, DEPTH)
    for i in range(early, SWEEPS):
        norms_ref[i : i + 1, :] = jnp.sqrt(total[i - early])


def put(x_ref, norms_ref, x_hbm, norms_hbm, sems):
    size = x_ref.shape[0] // 4
    copies = [pltpu.make_async_copy(norms_ref, norms_hbm, sems.at[4])]
    for i in range(4):
        rows = pl.ds(i * size, size)
        copies.append(pltpu.make_async_copy(x_ref.at[rows], x_hbm.at[rows], sems.at[i]))
    for copy in copies:
        copy.start()
    for copy in copies:
        copy.wait()


def solution(mesh):
    n = mesh.shape["row"]
    members = n // DEPTH

    def step(diag_blocks, lower_coupling, upper_coupling, right_sides):
        size, width = lower_coupling.shape
        cols = right_sides.shape[1]
        chunk = cols // CHUNKS
        last = SWEEPS - 1
        dma = pltpu.SemaphoreType.DMA
        halo = pltpu.VMEM((last, CHUNKS, width, chunk), F32)
        square = pltpu.VMEM((width, 2 * width), F32)
        row = lambda count: pltpu.VMEM((count, 1, cols), F32)
        results = pl.pallas_call(
            functools.partial(kernel, n),
            out_shape=(
                jax.ShapeDtypeStruct((size, cols), F32),
                jax.ShapeDtypeStruct((SWEEPS, cols), F32),
            ),
            in_specs=[pl.BlockSpec(memory_space=pltpu.HBM)] * 4,
            out_specs=(pl.BlockSpec(memory_space=pltpu.VMEM), pl.BlockSpec(memory_space=pltpu.VMEM)),
            scratch_shapes=[
                pltpu.VMEM((size, size), F32),
                pltpu.VMEM((width, size), F32),
                pltpu.VMEM((width, size), F32),
                pltpu.VMEM((size, cols), F32),
                pltpu.VMEM((size, size // 4), F32),
                pltpu.VMEM((size, size // 4), F32),
                pltpu.VMEM((size, 3 * size), BF16),
                pltpu.VMEM((size, 8 * width), BF16),
                pltpu.VMEM((width, 4 * width), BF16),
                pltpu.VMEM((width, 4 * width), BF16),
                pltpu.VMEM((CHUNKS, 2 * size, chunk), BF16),
                pltpu.VMEM((CHUNKS, 4 * width, chunk), BF16),
                pltpu.VMEM((CHUNKS, 4 * width, chunk), BF16),
                pltpu.VMEM((CHUNKS, size, chunk), F32),
                pltpu.VMEM((CHUNKS, width, chunk), F32),
                pltpu.VMEM((CHUNKS, width, chunk), F32),
                halo, halo, halo, halo,
                square, square, square, square,
                row(SWEEPS), row(members), row(DEPTH), row(members),
                pltpu.VMEM((members, 2, 1, cols), F32), pltpu.VMEM((DEPTH, 2, 1, cols), F32),
                dma((10,)),
                dma((last, CHUNKS)), dma((last, CHUNKS)), dma((last, CHUNKS)), dma((last, CHUNKS)), dma((4,)),
                dma((members,)), dma((members,)), dma((DEPTH,)), dma((DEPTH,)), dma((members,)), dma((members,)),
                dma((members,)), dma((members,)), dma((DEPTH,)), dma((DEPTH,)),
                pltpu.SemaphoreType.REGULAR, pltpu.SemaphoreType.REGULAR,
            ],
            compiler_params=pltpu.CompilerParams(
                collective_id=0, has_side_effects=True, vmem_limit_bytes=40 * 1024 * 1024
            ),
        )(*(
            pltpu.with_memory_space_constraint(array, pltpu.HBM)
            for array in (diag_blocks, lower_coupling.T, upper_coupling.T, right_sides)
        ))
        return pl.pallas_call(
            put,
            out_shape=tuple(jax.ShapeDtypeStruct(array.shape, F32) for array in results),
            in_specs=[pl.BlockSpec(memory_space=pltpu.VMEM)] * 2,
            out_specs=(pl.BlockSpec(memory_space=pltpu.HBM),) * 2,
            scratch_shapes=[dma((5,))],
            compiler_params=pltpu.CompilerParams(vmem_limit_bytes=1024 * 1024),
        )(*results)

    return jax.shard_map(
        step,
        mesh=mesh,
        in_specs=(P("row", None), P("row", None), P("row", None), P("row", "grp")),
        out_specs=(P("row", "grp"), P(None, "grp")),
        check_vma=False,
    )
```

```python
import functools

import jax
import jax.numpy as jnp
from jax import lax
from jax.experimental import pallas as pl
from jax.experimental.pallas import tpu as pltpu
from jax.sharding import PartitionSpec as P

MESH = pl.DeviceIdType.MESH
SWEEPS = 8
DEPTH = 16
CORES = 2
CHUNKS = 2
F32 = jnp.float32
BF16 = jnp.bfloat16


def split(value):
    hi = value.astype(BF16)
    return hi, (value - hi.astype(F32)).astype(BF16)


def dot(left, right):
    return jnp.dot(left, right, preferred_element_type=F32)


def kernel(
    n, diag_hbm, lower_hbm, upper_hbm, rhs_hbm, x_acc, norms_ref,
    diag, lower, upper, rhs, recip, pivot, mats, edges, gmat_in, gmat_out, parts, ends_in, ends_out, inner_z,
    add_in, add_out, send_in, recv_in, send_out, recv_out, gsend_in, grecv_in, gsend_out, grecv_out,
    sums, early_plane, early_line, early_rows, late_plane, late_line,
    load_sem, si_sem, ri_sem, so_sem, ro_sem, g_sem,
    ap_send, ap_recv, bp_send, bp_recv, cp_send, cp_recv, al_send, al_recv, bl_send, bl_recv, know_a, know_b,
):
    width, size = lower_hbm.shape
    cols = rhs_hbm.shape[1]
    chunk = cols // CHUNKS
    last = SWEEPS - 1
    early = SWEEPS - 2
    me = lax.axis_index("row")
    core = lax.rem(me, CORES)
    chip = lax.div(me, CORES)
    depth = lax.rem(chip, DEPTH)
    plane = lax.div(chip, DEPTH)
    planes = n // (CORES * DEPTH)
    members = planes * CORES
    place = plane * CORES + core
    near = me + 1 - 2 * core
    far = me - 1 + 2 * core
    has_far = jnp.logical_and(far >= 0, far < n)
    far_rows = pl.multiple_of(core * (size - width), width)
    near_rows = pl.multiple_of((1 - core) * (size - width), width)

    def at_place(other):
        return (lax.div(other, CORES) * DEPTH + depth) * CORES + lax.rem(other, CORES)

    def at_depth(other):
        return (plane * DEPTH + other) * CORES + core

    def signal(sem, target):
        pl.semaphore_signal(sem, inc=1, device_id={"row": target}, device_id_type=MESH)

    def remote(src, dst, send_sem, recv_sem, target):
        return pltpu.make_async_remote_copy(
            src_ref=src, dst_ref=dst, send_sem=send_sem, recv_sem=recv_sem,
            device_id={"row": target}, device_id_type=MESH,
        )

    slab = size // 4
    loads = []

    def load(src, dst):
        copy = pltpu.make_async_copy(src, dst, load_sem.at[len(loads)])
        copy.start()
        loads.append(copy)
        return copy

    diag_loads, rhs_loads = {}, {}
    for i in (0, 3):
        diag_loads[i] = load(diag_hbm.at[pl.ds(i * slab, slab)], diag.at[pl.ds(i * slab, slab)])
        rhs_loads[i] = load(rhs_hbm.at[pl.ds(i * slab, slab)], rhs.at[pl.ds(i * slab, slab)])
    lower_load = load(lower_hbm, lower)
    upper_load = load(upper_hbm, upper)
    for i in (1, 2):
        diag_loads[i] = load(diag_hbm.at[pl.ds(i * slab, slab)], diag.at[pl.ds(i * slab, slab)])
        rhs_loads[i] = load(rhs_hbm.at[pl.ds(i * slab, slab)], rhs.at[pl.ds(i * slab, slab)])

    barrier = pltpu.get_barrier_semaphore()
    for offset in range(1, members):
        signal(barrier, at_place(lax.rem(place + offset, members)))
    for offset in (1, 2, DEPTH - 2, DEPTH - 1):
        signal(barrier, at_depth(lax.rem(depth + offset, DEPTH)))

    @pl.when(has_far)
    def _():
        signal(barrier, far)

    @pl.when(jnp.logical_not(has_far))
    def _():
        recv_out[...] = jnp.zeros_like(recv_out)
        grecv_out[...] = jnp.zeros_like(grecv_out)

    add_in[...] = jnp.zeros_like(add_in)
    add_out[...] = jnp.zeros_like(add_out)

    mask = lax.broadcasted_iota(jnp.int32, (slab, slab), 0) == lax.broadcasted_iota(jnp.int32, (slab, slab), 1)

    def pivots(i):
        rows = pl.ds(i * slab, slab)
        block = diag[rows, pl.ds(i * slab, slab)]
        values = jnp.sum(jnp.where(mask, block, 0.0), axis=1, keepdims=True)
        pivot[rows, :] = jnp.broadcast_to(values, (slab, slab))
        first = 1.0 / values
        recip[rows, :] = jnp.broadcast_to(first + first * (1.0 - values * first), (slab, slab))

    def scale(block, rows):
        factor = recip[rows, :]
        return jnp.concatenate([block[:, j : j + slab] * factor for j in range(0, block.shape[1], slab)], axis=1)

    for i in (0, 3):
        diag_loads[i].wait()
        pivots(i)
    for i in (0, 3):
        rhs_loads[i].wait()
    for ch in range(CHUNKS):
        span = pl.ds(ch * chunk, chunk)
        near_slice, far_slice = pl.ds(near_rows, width), pl.ds(far_rows, width)
        send_out[0, ch] = scale(rhs[far_slice, span], far_slice)
        send_in[0, ch] = scale(rhs[near_slice, span], near_slice)

    @pl.when(has_far)
    def _():
        pl.semaphore_wait(barrier, members + 4)

    @pl.when(jnp.logical_not(has_far))
    def _():
        pl.semaphore_wait(barrier, members + 3)

    def near_copy(s, ch):
        return remote(send_in.at[s, ch], recv_in.at[s, ch], si_sem.at[s, ch], ri_sem.at[s, ch], near)

    def far_copy(s, ch):
        return remote(send_out.at[s, ch], recv_out.at[s, ch], so_sem.at[s, ch], ro_sem.at[s, ch], far)

    def g_copy_near():
        return remote(gsend_in, grecv_in, g_sem.at[0], g_sem.at[1], near)

    def g_copy_far():
        return remote(gsend_out, grecv_out, g_sem.at[2], g_sem.at[3], far)

    def if_far(action):
        @pl.when(has_far)
        def _():
            action()

    for ch in range(CHUNKS):
        if_far(lambda ch=ch: far_copy(0, ch).start())
        near_copy(0, ch).start()
    signal(know_a, at_depth(lax.rem(depth + 2, DEPTH)))
    signal(know_a, at_depth(lax.rem(depth + DEPTH - 2, DEPTH)))

    for i in (1, 2):
        diag_loads[i].wait()
        pivots(i)
    lower_load.wait()
    upper_load.wait()
    for i in range(4):
        rows = pl.ds(i * slab, slab)
        low, up = lower[:, rows].T, upper[:, rows].T
        to_near = jnp.where(core == 0, up, low)
        to_far = jnp.where(has_far, jnp.where(core == 0, low, up), 0.0)
        for position, block in enumerate((to_near, to_far)):
            twice = jnp.concatenate([block, block], axis=1) * (-recip[rows, :])
            hi, lo = split(twice)
            edges[rows, pl.ds(position * 2 * slab, slab)] = hi
            edges[rows, pl.ds(position * 2 * slab + slab, slab)] = lo

    def rejoin(rows, position):
        hi = edges[rows, pl.ds(position * 2 * slab, slab)].astype(F32)
        return hi + edges[rows, pl.ds(position * 2 * slab + slab, slab)].astype(F32)

    gsend_in[...] = rejoin(pl.ds(near_rows, width), 0)
    gsend_out[...] = rejoin(pl.ds(far_rows, width), 1)
    if_far(lambda: g_copy_far().start())
    g_copy_near().start()

    for i in range(4):
        rows = pl.ds(i * slab, slab)
        factor = -recip[rows, :]
        for j in range(4):
            block = diag[rows, pl.ds(j * slab, slab)]
            if i == j:
                block = jnp.where(mask, 0.0, block)
            hi, lo = split(block * factor)
            mats[rows, pl.ds(j * slab, slab)] = hi
            mats[rows, pl.ds(size + j * slab, slab)] = hi
            mats[rows, pl.ds(2 * size + j * slab, slab)] = lo

    for i in (1, 2):
        rhs_loads[i].wait()

    tile = 64

    def rows_sum(total):
        return jnp.sum(total, axis=0, keepdims=True)

    def keep(ch, r, value):
        hi, lo = split(value)
        parts[ch, pl.ds(r, tile), :] = hi
        parts[ch, pl.ds(size + r, tile), :] = lo

    def begin(ch):
        span = pl.ds(ch * chunk, chunk)
        total = jnp.zeros((8, chunk), F32)
        for r in range(0, size, tile):
            rows = pl.ds(r, tile)
            block = rhs[rows, span]
            total += jnp.sum((block * block).reshape(tile // 8, 8, chunk), axis=0)
            value = scale(block, rows)
            x_acc[rows, span] = value
            keep(ch, r, value)
        sums[0, :, span] = rows_sum(total)

    def advance(ch):
        low_high = parts[ch]
        right = jnp.concatenate([low_high, low_high[:size]], axis=0)
        for r in range(0, size, size // 2):
            inner_z[ch, pl.ds(r, size // 2), :] = dot(mats[pl.ds(r, size // 2), :], right)

    def echo(ch):
        for rows, gmat, add in ((near_rows, gmat_in, add_in), (far_rows, gmat_out, add_out)):
            hi = parts[ch, pl.ds(rows, width), :]
            lo = parts[ch, pl.ds(size + rows, width), :]
            add[ch] = dot(gmat[...], jnp.concatenate([hi, lo, hi, lo], axis=0))

    def take(ch, received, add, ends):
        hi, lo = split(received + add[ch])
        ends[ch] = jnp.concatenate([hi, lo, hi, lo], axis=0)

    def from_near(s, ch, send):
        near_copy(s, ch).wait_recv()
        take(ch, recv_in[s, ch], add_in, ends_in)
        if send:
            rows = pl.ds(far_rows, width)
            send_out[s + 1, ch] = inner_z[ch, rows, :] + dot(edges[rows, : 2 * slab], ends_in[ch])
            if_far(lambda: far_copy(s + 1, ch).start())

    def from_far(s, ch, send):
        if_far(lambda: far_copy(s, ch).wait_recv())
        take(ch, recv_out[s, ch], add_out, ends_out)
        if send:
            rows = pl.ds(near_rows, width)
            send_in[s + 1, ch] = inner_z[ch, rows, :] + dot(edges[rows, 2 * slab :], ends_out[ch])
            near_copy(s + 1, ch).start()

    def complete(s, ch, final):
        span = pl.ds(ch * chunk, chunk)
        right = jnp.concatenate([ends_in[ch], ends_out[ch]], axis=0)
        for r in range(0, size, size // 2):
            inner_z[ch, pl.ds(r, size // 2), :] += dot(edges[pl.ds(r, size // 2), :], right)
        total = jnp.zeros((8, chunk), F32)
        for r in range(0, size, tile):
            rows = pl.ds(r, tile)
            value = inner_z[ch, rows, :]
            x_acc[rows, span] += value
            if not final:
                keep(ch, r, value)
            factor = pivot[rows, :]
            residual = jnp.concatenate([value[:, j : j + slab] * factor for j in range(0, chunk, slab)], axis=1)
            total += jnp.sum((residual * residual).reshape(tile // 8, 8, chunk), axis=0)
        sums[s + 1, :, span] = rows_sum(total)

    for ch in range(CHUNKS):
        begin(ch)
        advance(ch)

    def take_squares():
        g_copy_near().wait_recv()
        if_far(lambda: g_copy_far().wait_recv())
        for source, target in ((grecv_in, gmat_in), (grecv_out, gmat_out)):
            hi, lo = split(source[...])
            target[:, :slab] = hi
            target[:, slab:] = lo

    def sweep(s):
        for ch in range(CHUNKS):
            from_far(s, ch, True)
            if ch > 0:
                from_near(s + 1, ch - 1, s + 1 < last - 1)
            elif s == 0:
                take_squares()
            echo(ch)
            complete(s, ch, False)
            advance(ch)
        from_near(s + 1, CHUNKS - 1, s + 1 < last - 1)

    def early_a(offset, target_place):
        return remote(
            sums.at[target_place], early_plane.at[place], ap_send.at[offset], ap_recv.at[offset], at_place(target_place)
        )

    def line(buffer, send_sem, recv_sem, offset):
        return remote(
            buffer.at[depth], buffer.at[depth], send_sem.at[offset], recv_sem.at[offset],
            at_depth(lax.rem(depth + offset, DEPTH)),
        )

    def late_a(offset):
        return remote(
            sums.at[pl.ds(early, SWEEPS - early)], late_plane.at[place], al_send.at[offset], al_recv.at[offset],
            at_place(lax.rem(place + offset, members)),
        )

    def early_c(offset):
        return remote(
            early_rows.at[place], early_rows.at[place], cp_send.at[offset], cp_recv.at[offset],
            at_place(lax.rem(place + offset, members)),
        )

    def added(buffer, count):
        values = [buffer[i] for i in range(count)]
        while len(values) > 1:
            values = [values[i] + values[i + 1] for i in range(0, len(values), 2)]
        return values[0]

    for ch in range(CHUNKS):
        from_near(0, ch, True)
    for s in range(early - 1):
        sweep(s)

    for offset in range(1, members):
        target_place = lax.rem(place + offset, members)

        @pl.when(target_place < early)
        def _(offset=offset, target_place=target_place):
            early_a(offset, target_place).start()

    pl.semaphore_wait(know_a, 2)
    signal(know_b, at_depth(lax.rem(depth + 4, DEPTH)))
    signal(know_b, at_depth(lax.rem(depth + DEPTH - 4, DEPTH)))
    for s in range(early - 1, last - 1):
        sweep(s)
    pl.semaphore_wait(know_b, 2)

    @pl.when(place < early)
    def _():
        early_plane[place] = sums[place]
        for offset in range(1, members):
            early_a(offset, place).wait_recv()
        early_line[depth] = added(early_plane, members)
        for offset in range(1, DEPTH):
            line(early_line, bp_send, bp_recv, offset).start()

    for ch in range(CHUNKS):
        from_far(last - 1, ch, False)
        complete(last - 1, ch, True)

    for offset in range(1, members):
        late_a(offset).start()
    late_plane[place] = sums[early:]

    for s in range(last):
        for ch in range(CHUNKS):
            near_copy(s, ch).wait_send()
            if_far(lambda s=s, ch=ch: far_copy(s, ch).wait_send())
    g_copy_near().wait_send()
    if_far(lambda: g_copy_far().wait_send())
    for offset in range(1, members):

        @pl.when(lax.rem(place + offset, members) < early)
        def _(offset=offset):
            early_a(offset, place).wait_send()

    for offset in range(1, members):
        late_a(offset).wait_recv()
    late_line[depth] = added(late_plane, members)
    for offset in range(1, DEPTH):
        line(late_line, bl_send, bl_recv, offset).start()

    @pl.when(place < early)
    def _():
        for offset in range(1, DEPTH):
            line(early_line, bp_send, bp_recv, offset).wait_recv()
        early_rows[place] = added(early_line, DEPTH)
        for offset in range(1, members):
            early_c(offset).start()

    for offset in range(1, members):

        @pl.when(lax.rem(place + members - offset, members) < early)
        def _(offset=offset):
            early_c(offset).wait_recv()

    for i in range(early):
        norms_ref[i : i + 1, :] = jnp.sqrt(early_rows[i])
    for offset in range(1, members):
        late_a(offset).wait_send()

    @pl.when(place < early)
    def _():
        for offset in range(1, DEPTH):
            line(early_line, bp_send, bp_recv, offset).wait_send()
        for offset in range(1, members):
            early_c(offset).wait_send()

    for offset in range(1, DEPTH):
        line(late_line, bl_send, bl_recv, offset).wait_send()
    for offset in range(1, DEPTH):
        line(late_line, bl_send, bl_recv, offset).wait_recv()
    total = added(late_line, DEPTH)
    for i in range(early, SWEEPS):
        norms_ref[i : i + 1, :] = jnp.sqrt(total[i - early])


def put(x_ref, norms_ref, x_hbm, norms_hbm, sems):
    size = x_ref.shape[0] // 4
    copies = [pltpu.make_async_copy(norms_ref, norms_hbm, sems.at[4])]
    for i in range(4):
        rows = pl.ds(i * size, size)
        copies.append(pltpu.make_async_copy(x_ref.at[rows], x_hbm.at[rows], sems.at[i]))
    for copy in copies:
        copy.start()
    for copy in copies:
        copy.wait()


def solution(mesh):
    n = mesh.shape["row"]
    members = n // DEPTH

    def step(diag_blocks, lower_coupling, upper_coupling, right_sides):
        size, width = lower_coupling.shape
        cols = right_sides.shape[1]
        chunk = cols // CHUNKS
        last = SWEEPS - 1
        dma = pltpu.SemaphoreType.DMA
        halo = pltpu.VMEM((last, CHUNKS, width, chunk), F32)
        square = pltpu.VMEM((width, 2 * width), F32)
        row = lambda count: pltpu.VMEM((count, 1, cols), F32)
        results = pl.pallas_call(
            functools.partial(kernel, n),
            out_shape=(
                jax.ShapeDtypeStruct((size, cols), F32),
                jax.ShapeDtypeStruct((SWEEPS, cols), F32),
            ),
            in_specs=[pl.BlockSpec(memory_space=pltpu.HBM)] * 4,
            out_specs=(pl.BlockSpec(memory_space=pltpu.VMEM), pl.BlockSpec(memory_space=pltpu.VMEM)),
            scratch_shapes=[
                pltpu.VMEM((size, size), F32),
                pltpu.VMEM((width, size), F32),
                pltpu.VMEM((width, size), F32),
                pltpu.VMEM((size, cols), F32),
                pltpu.VMEM((size, size // 4), F32),
                pltpu.VMEM((size, size // 4), F32),
                pltpu.VMEM((size, 3 * size), BF16),
                pltpu.VMEM((size, 8 * width), BF16),
                pltpu.VMEM((width, 4 * width), BF16),
                pltpu.VMEM((width, 4 * width), BF16),
                pltpu.VMEM((CHUNKS, 2 * size, chunk), BF16),
                pltpu.VMEM((CHUNKS, 4 * width, chunk), BF16),
                pltpu.VMEM((CHUNKS, 4 * width, chunk), BF16),
                pltpu.VMEM((CHUNKS, size, chunk), F32),
                pltpu.VMEM((CHUNKS, width, chunk), F32),
                pltpu.VMEM((CHUNKS, width, chunk), F32),
                halo, halo, halo, halo,
                square, square, square, square,
                row(SWEEPS), row(members), row(DEPTH), row(members),
                pltpu.VMEM((members, 2, 1, cols), F32), pltpu.VMEM((DEPTH, 2, 1, cols), F32),
                dma((10,)),
                dma((last, CHUNKS)), dma((last, CHUNKS)), dma((last, CHUNKS)), dma((last, CHUNKS)), dma((4,)),
                dma((members,)), dma((members,)), dma((DEPTH,)), dma((DEPTH,)), dma((members,)), dma((members,)),
                dma((members,)), dma((members,)), dma((DEPTH,)), dma((DEPTH,)),
                pltpu.SemaphoreType.REGULAR, pltpu.SemaphoreType.REGULAR,
            ],
            compiler_params=pltpu.CompilerParams(
                collective_id=0, has_side_effects=True, vmem_limit_bytes=40 * 1024 * 1024
            ),
        )(*(
            pltpu.with_memory_space_constraint(array, pltpu.HBM)
            for array in (diag_blocks, lower_coupling.T, upper_coupling.T, right_sides)
        ))
        return pl.pallas_call(
            put,
            out_shape=tuple(jax.ShapeDtypeStruct(array.shape, F32) for array in results),
            in_specs=[pl.BlockSpec(memory_space=pltpu.VMEM)] * 2,
            out_specs=(pl.BlockSpec(memory_space=pltpu.HBM),) * 2,
            scratch_shapes=[dma((5,))],
            compiler_params=pltpu.CompilerParams(vmem_limit_bytes=1024 * 1024),
        )(*results)

    return jax.shard_map(
        step,
        mesh=mesh,
        in_specs=(P("row", None), P("row", None), P("row", None), P("row", "grp")),
        out_specs=(P("row", "grp"), P(None, "grp")),
        check_vma=False,
    )
```

```python
import functools

import jax
import jax.numpy as jnp
from jax import lax
from jax.experimental import pallas as pl
from jax.experimental.pallas import tpu as pltpu
from jax.sharding import PartitionSpec as P

MESH = pl.DeviceIdType.MESH
SWEEPS = 8
DEPTH = 16
CORES = 2
CHUNKS = 2
F32 = jnp.float32
BF16 = jnp.bfloat16


def split(value):
    hi = value.astype(BF16)
    return hi, (value - hi.astype(F32)).astype(BF16)


def dot(left, right):
    return jnp.dot(left, right, preferred_element_type=F32)


def kernel(
    n, diag_hbm, lower_hbm, upper_hbm, rhs_hbm, x_acc, norms_ref,
    diag, lower, upper, rhs, recip, pivot, mats, edges, gmat_in, gmat_out, parts, ends_in, ends_out, inner_z,
    add_in, add_out, send_in, recv_in, send_out, recv_out, gsend_in, grecv_in, gsend_out, grecv_out,
    sums, early_plane, early_line, early_rows, late_plane, late_line,
    load_sem, si_sem, ri_sem, so_sem, ro_sem, g_sem,
    ap_send, ap_recv, bp_send, bp_recv, cp_send, cp_recv, al_send, al_recv, bl_send, bl_recv, know_a, know_b,
):
    width, size = lower_hbm.shape
    cols = rhs_hbm.shape[1]
    chunk = cols // CHUNKS
    last = SWEEPS - 1
    early = SWEEPS - 2
    me = lax.axis_index("row")
    core = lax.rem(me, CORES)
    chip = lax.div(me, CORES)
    depth = lax.rem(chip, DEPTH)
    plane = lax.div(chip, DEPTH)
    planes = n // (CORES * DEPTH)
    members = planes * CORES
    place = plane * CORES + core
    near = me + 1 - 2 * core
    far = me - 1 + 2 * core
    has_far = jnp.logical_and(far >= 0, far < n)
    far_rows = pl.multiple_of(core * (size - width), width)
    near_rows = pl.multiple_of((1 - core) * (size - width), width)

    def at_place(other):
        return (lax.div(other, CORES) * DEPTH + depth) * CORES + lax.rem(other, CORES)

    def at_depth(other):
        return (plane * DEPTH + other) * CORES + core

    def signal(sem, target):
        pl.semaphore_signal(sem, inc=1, device_id={"row": target}, device_id_type=MESH)

    def remote(src, dst, send_sem, recv_sem, target):
        return pltpu.make_async_remote_copy(
            src_ref=src, dst_ref=dst, send_sem=send_sem, recv_sem=recv_sem,
            device_id={"row": target}, device_id_type=MESH,
        )

    slab = size // 4
    loads = []

    def load(src, dst):
        copy = pltpu.make_async_copy(src, dst, load_sem.at[len(loads)])
        copy.start()
        loads.append(copy)
        return copy

    diag_loads, rhs_loads = {}, {}
    for i in (0, 3):
        diag_loads[i] = load(diag_hbm.at[pl.ds(i * slab, slab)], diag.at[pl.ds(i * slab, slab)])
        rhs_loads[i] = load(rhs_hbm.at[pl.ds(i * slab, slab)], rhs.at[pl.ds(i * slab, slab)])
    lower_load = load(lower_hbm, lower)
    upper_load = load(upper_hbm, upper)
    for i in (1, 2):
        diag_loads[i] = load(diag_hbm.at[pl.ds(i * slab, slab)], diag.at[pl.ds(i * slab, slab)])
        rhs_loads[i] = load(rhs_hbm.at[pl.ds(i * slab, slab)], rhs.at[pl.ds(i * slab, slab)])

    barrier = pltpu.get_barrier_semaphore()
    for offset in range(1, members):
        signal(barrier, at_place(lax.rem(place + offset, members)))
    for offset in (1, 2, DEPTH - 2, DEPTH - 1):
        signal(barrier, at_depth(lax.rem(depth + offset, DEPTH)))

    @pl.when(has_far)
    def _():
        signal(barrier, far)

    @pl.when(jnp.logical_not(has_far))
    def _():
        recv_out[...] = jnp.zeros_like(recv_out)
        grecv_out[...] = jnp.zeros_like(grecv_out)

    add_in[...] = jnp.zeros_like(add_in)
    add_out[...] = jnp.zeros_like(add_out)

    mask = lax.broadcasted_iota(jnp.int32, (slab, slab), 0) == lax.broadcasted_iota(jnp.int32, (slab, slab), 1)

    def pivots(i):
        rows = pl.ds(i * slab, slab)
        block = diag[rows, pl.ds(i * slab, slab)]
        values = jnp.sum(jnp.where(mask, block, 0.0), axis=1, keepdims=True)
        pivot[rows, :] = jnp.broadcast_to(values, (slab, slab))
        first = 1.0 / values
        recip[rows, :] = jnp.broadcast_to(first + first * (1.0 - values * first), (slab, slab))

    def scale(block, rows):
        factor = recip[rows, :]
        return jnp.concatenate([block[:, j : j + slab] * factor for j in range(0, block.shape[1], slab)], axis=1)

    for i in (0, 3):
        diag_loads[i].wait()
        pivots(i)
    for i in (0, 3):
        rhs_loads[i].wait()
    for ch in range(CHUNKS):
        span = pl.ds(ch * chunk, chunk)
        near_slice, far_slice = pl.ds(near_rows, width), pl.ds(far_rows, width)
        send_out[0, ch] = scale(rhs[far_slice, span], far_slice)
        send_in[0, ch] = scale(rhs[near_slice, span], near_slice)

    @pl.when(has_far)
    def _():
        pl.semaphore_wait(barrier, members + 4)

    @pl.when(jnp.logical_not(has_far))
    def _():
        pl.semaphore_wait(barrier, members + 3)

    def near_copy(s, ch):
        return remote(send_in.at[s, ch], recv_in.at[s, ch], si_sem.at[s, ch], ri_sem.at[s, ch], near)

    def far_copy(s, ch):
        return remote(send_out.at[s, ch], recv_out.at[s, ch], so_sem.at[s, ch], ro_sem.at[s, ch], far)

    def g_copy_near():
        return remote(gsend_in, grecv_in, g_sem.at[0], g_sem.at[1], near)

    def g_copy_far():
        return remote(gsend_out, grecv_out, g_sem.at[2], g_sem.at[3], far)

    def if_far(action):
        @pl.when(has_far)
        def _():
            action()

    for ch in range(CHUNKS):
        if_far(lambda ch=ch: far_copy(0, ch).start())
        near_copy(0, ch).start()
    signal(know_a, at_depth(lax.rem(depth + 2, DEPTH)))
    signal(know_a, at_depth(lax.rem(depth + DEPTH - 2, DEPTH)))

    for i in (1, 2):
        diag_loads[i].wait()
        pivots(i)
    lower_load.wait()
    upper_load.wait()
    for i in range(4):
        rows = pl.ds(i * slab, slab)
        low, up = lower[:, rows].T, upper[:, rows].T
        to_near = jnp.where(core == 0, up, low)
        to_far = jnp.where(has_far, jnp.where(core == 0, low, up), 0.0)
        for position, block in enumerate((to_near, to_far)):
            twice = jnp.concatenate([block, block], axis=1) * (-recip[rows, :])
            hi, lo = split(twice)
            edges[rows, pl.ds(position * 2 * slab, slab)] = hi
            edges[rows, pl.ds(position * 2 * slab + slab, slab)] = lo

    def rejoin(rows, position):
        hi = edges[rows, pl.ds(position * 2 * slab, slab)].astype(F32)
        return hi + edges[rows, pl.ds(position * 2 * slab + slab, slab)].astype(F32)

    gsend_in[...] = rejoin(pl.ds(near_rows, width), 0)
    gsend_out[...] = rejoin(pl.ds(far_rows, width), 1)
    if_far(lambda: g_copy_far().start())
    g_copy_near().start()

    for i in range(4):
        rows = pl.ds(i * slab, slab)
        factor = -recip[rows, :]
        for j in range(4):
            block = diag[rows, pl.ds(j * slab, slab)]
            if i == j:
                block = jnp.where(mask, 0.0, block)
            hi, lo = split(block * factor)
            mats[rows, pl.ds(j * slab, slab)] = hi
            mats[rows, pl.ds(size + j * slab, slab)] = hi
            mats[rows, pl.ds(2 * size + j * slab, slab)] = lo

    for i in (1, 2):
        rhs_loads[i].wait()

    tile = 64

    def rows_sum(total):
        return jnp.sum(total, axis=0, keepdims=True)

    def keep(ch, r, value):
        hi, lo = split(value)
        parts[ch, pl.ds(r, tile), :] = hi
        parts[ch, pl.ds(size + r, tile), :] = lo

    def begin(ch):
        span = pl.ds(ch * chunk, chunk)
        total = jnp.zeros((8, chunk), F32)
        for r in range(0, size, tile):
            rows = pl.ds(r, tile)
            block = rhs[rows, span]
            total += jnp.sum((block * block).reshape(tile // 8, 8, chunk), axis=0)
            value = scale(block, rows)
            x_acc[rows, span] = value
            keep(ch, r, value)
        sums[0, :, span] = rows_sum(total)

    def advance(ch):
        low_high = parts[ch]
        right = jnp.concatenate([low_high, low_high[:size]], axis=0)
        for r in range(0, size, size // 2):
            inner_z[ch, pl.ds(r, size // 2), :] = dot(mats[pl.ds(r, size // 2), :], right)

    def echo(ch):
        for rows, gmat, add in ((near_rows, gmat_in, add_in), (far_rows, gmat_out, add_out)):
            hi = parts[ch, pl.ds(rows, width), :]
            lo = parts[ch, pl.ds(size + rows, width), :]
            add[ch] = dot(gmat[...], jnp.concatenate([hi, lo, hi, lo], axis=0))

    def take(ch, received, add, ends):
        hi, lo = split(received + add[ch])
        ends[ch] = jnp.concatenate([hi, lo, hi, lo], axis=0)

    def from_near(s, ch, send):
        near_copy(s, ch).wait_recv()
        take(ch, recv_in[s, ch], add_in, ends_in)
        if send:
            rows = pl.ds(far_rows, width)
            send_out[s + 1, ch] = inner_z[ch, rows, :] + dot(edges[rows, : 2 * slab], ends_in[ch])
            if_far(lambda: far_copy(s + 1, ch).start())

    def from_far(s, ch, send):
        if_far(lambda: far_copy(s, ch).wait_recv())
        take(ch, recv_out[s, ch], add_out, ends_out)
        if send:
            rows = pl.ds(near_rows, width)
            send_in[s + 1, ch] = inner_z[ch, rows, :] + dot(edges[rows, 2 * slab :], ends_out[ch])
            near_copy(s + 1, ch).start()

    def complete(s, ch, final):
        span = pl.ds(ch * chunk, chunk)
        right = jnp.concatenate([ends_in[ch], ends_out[ch]], axis=0)
        total = jnp.zeros((8, chunk), F32)
        for start in range(0, size, size // 2):
            half = pl.ds(start, size // 2)
            block = inner_z[ch, half, :] + dot(edges[half, :], right)
            for r in range(0, size // 2, tile):
                rows = pl.ds(start + r, tile)
                value = block[r : r + tile]
                x_acc[rows, span] += value
                if not final:
                    keep(ch, start + r, value)
                factor = pivot[rows, :]
                residual = jnp.concatenate([value[:, j : j + slab] * factor for j in range(0, chunk, slab)], axis=1)
                total += jnp.sum((residual * residual).reshape(tile // 8, 8, chunk), axis=0)
        sums[s + 1, :, span] = rows_sum(total)

    for ch in range(CHUNKS):
        begin(ch)
        advance(ch)

    def take_squares():
        g_copy_near().wait_recv()
        if_far(lambda: g_copy_far().wait_recv())
        for source, target in ((grecv_in, gmat_in), (grecv_out, gmat_out)):
            hi, lo = split(source[...])
            target[:, :slab] = hi
            target[:, slab:] = lo

    def sweep(s):
        for ch in range(CHUNKS):
            from_far(s, ch, True)
            if ch > 0:
                from_near(s + 1, ch - 1, s + 1 < last - 1)
            elif s == 0:
                take_squares()
            echo(ch)
            complete(s, ch, False)
            advance(ch)
        from_near(s + 1, CHUNKS - 1, s + 1 < last - 1)

    def early_a(offset, target_place):
        return remote(
            sums.at[target_place], early_plane.at[place], ap_send.at[offset], ap_recv.at[offset], at_place(target_place)
        )

    def line(buffer, send_sem, recv_sem, offset):
        return remote(
            buffer.at[depth], buffer.at[depth], send_sem.at[offset], recv_sem.at[offset],
            at_depth(lax.rem(depth + offset, DEPTH)),
        )

    def late_a(i, offset):
        return remote(
            sums.at[early + i], late_plane.at[i, place], al_send.at[i, offset], al_recv.at[i, offset],
            at_place(lax.rem(place + offset, members)),
        )

    def late_b(i, offset):
        return line(late_line.at[i], bl_send.at[i], bl_recv.at[i], offset)

    def late_row(i):
        for offset in range(1, members):
            late_a(i, offset).start()
        late_plane[i, place] = sums[early + i]

    def late_sum(i):
        for offset in range(1, members):
            late_a(i, offset).wait_recv()
        late_line[i, depth] = added(late_plane.at[i], members)
        for offset in range(1, DEPTH):
            late_b(i, offset).start()

    def early_c(offset):
        return remote(
            early_rows.at[place], early_rows.at[place], cp_send.at[offset], cp_recv.at[offset],
            at_place(lax.rem(place + offset, members)),
        )

    def added(buffer, count):
        values = [buffer[i] for i in range(count)]
        while len(values) > 1:
            values = [values[i] + values[i + 1] for i in range(0, len(values), 2)]
        return values[0]

    for ch in range(CHUNKS):
        from_near(0, ch, True)
    for s in range(early - 1):
        sweep(s)

    for offset in range(1, members):
        target_place = lax.rem(place + offset, members)

        @pl.when(target_place < early)
        def _(offset=offset, target_place=target_place):
            early_a(offset, target_place).start()

    pl.semaphore_wait(know_a, 2)
    signal(know_b, at_depth(lax.rem(depth + 4, DEPTH)))
    signal(know_b, at_depth(lax.rem(depth + DEPTH - 4, DEPTH)))
    for s in range(early - 1, last - 1):
        sweep(s)
    late_row(0)
    pl.semaphore_wait(know_b, 2)

    @pl.when(place < early)
    def _():
        early_plane[place] = sums[place]
        for offset in range(1, members):
            early_a(offset, place).wait_recv()
        early_line[depth] = added(early_plane, members)
        for offset in range(1, DEPTH):
            line(early_line, bp_send, bp_recv, offset).start()

    for ch in range(CHUNKS):
        from_far(last - 1, ch, False)
        complete(last - 1, ch, True)

    late_row(1)

    for s in range(last):
        for ch in range(CHUNKS):
            near_copy(s, ch).wait_send()
            if_far(lambda s=s, ch=ch: far_copy(s, ch).wait_send())
    g_copy_near().wait_send()
    if_far(lambda: g_copy_far().wait_send())
    for offset in range(1, members):

        @pl.when(lax.rem(place + offset, members) < early)
        def _(offset=offset):
            early_a(offset, place).wait_send()

    for i in range(SWEEPS - early):
        late_sum(i)

    @pl.when(place < early)
    def _():
        for offset in range(1, DEPTH):
            line(early_line, bp_send, bp_recv, offset).wait_recv()
        early_rows[place] = added(early_line, DEPTH)
        for offset in range(1, members):
            early_c(offset).start()

    for offset in range(1, members):

        @pl.when(lax.rem(place + members - offset, members) < early)
        def _(offset=offset):
            early_c(offset).wait_recv()

    for i in range(early):
        norms_ref[i : i + 1, :] = jnp.sqrt(early_rows[i])
    for i in range(SWEEPS - early):
        for offset in range(1, members):
            late_a(i, offset).wait_send()

    @pl.when(place < early)
    def _():
        for offset in range(1, DEPTH):
            line(early_line, bp_send, bp_recv, offset).wait_send()
        for offset in range(1, members):
            early_c(offset).wait_send()

    for i in range(SWEEPS - early):
        for offset in range(1, DEPTH):
            late_b(i, offset).wait_send()
    for i in range(SWEEPS - early):
        for offset in range(1, DEPTH):
            late_b(i, offset).wait_recv()
        norms_ref[early + i : early + i + 1, :] = jnp.sqrt(added(late_line.at[i], DEPTH))


def put(x_ref, norms_ref, x_hbm, norms_hbm, sems):
    size = x_ref.shape[0] // 4
    copies = [pltpu.make_async_copy(norms_ref, norms_hbm, sems.at[4])]
    for i in range(4):
        rows = pl.ds(i * size, size)
        copies.append(pltpu.make_async_copy(x_ref.at[rows], x_hbm.at[rows], sems.at[i]))
    for copy in copies:
        copy.start()
    for copy in copies:
        copy.wait()


def solution(mesh):
    n = mesh.shape["row"]
    members = n // DEPTH

    def step(diag_blocks, lower_coupling, upper_coupling, right_sides):
        size, width = lower_coupling.shape
        cols = right_sides.shape[1]
        chunk = cols // CHUNKS
        last = SWEEPS - 1
        dma = pltpu.SemaphoreType.DMA
        halo = pltpu.VMEM((last, CHUNKS, width, chunk), F32)
        square = pltpu.VMEM((width, 2 * width), F32)
        row = lambda count: pltpu.VMEM((count, 1, cols), F32)
        results = pl.pallas_call(
            functools.partial(kernel, n),
            out_shape=(
                jax.ShapeDtypeStruct((size, cols), F32),
                jax.ShapeDtypeStruct((SWEEPS, cols), F32),
            ),
            in_specs=[pl.BlockSpec(memory_space=pltpu.HBM)] * 4,
            out_specs=(pl.BlockSpec(memory_space=pltpu.VMEM), pl.BlockSpec(memory_space=pltpu.VMEM)),
            scratch_shapes=[
                pltpu.VMEM((size, size), F32),
                pltpu.VMEM((width, size), F32),
                pltpu.VMEM((width, size), F32),
                pltpu.VMEM((size, cols), F32),
                pltpu.VMEM((size, size // 4), F32),
                pltpu.VMEM((size, size // 4), F32),
                pltpu.VMEM((size, 3 * size), BF16),
                pltpu.VMEM((size, 8 * width), BF16),
                pltpu.VMEM((width, 4 * width), BF16),
                pltpu.VMEM((width, 4 * width), BF16),
                pltpu.VMEM((CHUNKS, 2 * size, chunk), BF16),
                pltpu.VMEM((CHUNKS, 4 * width, chunk), BF16),
                pltpu.VMEM((CHUNKS, 4 * width, chunk), BF16),
                pltpu.VMEM((CHUNKS, size, chunk), F32),
                pltpu.VMEM((CHUNKS, width, chunk), F32),
                pltpu.VMEM((CHUNKS, width, chunk), F32),
                halo, halo, halo, halo,
                square, square, square, square,
                row(SWEEPS), row(members), row(DEPTH), row(members),
                pltpu.VMEM((2, members, 1, cols), F32), pltpu.VMEM((2, DEPTH, 1, cols), F32),
                dma((10,)),
                dma((last, CHUNKS)), dma((last, CHUNKS)), dma((last, CHUNKS)), dma((last, CHUNKS)), dma((4,)),
                dma((members,)), dma((members,)), dma((DEPTH,)), dma((DEPTH,)), dma((members,)), dma((members,)),
                dma((2, members)), dma((2, members)), dma((2, DEPTH)), dma((2, DEPTH)),
                pltpu.SemaphoreType.REGULAR, pltpu.SemaphoreType.REGULAR,
            ],
            compiler_params=pltpu.CompilerParams(
                collective_id=0, has_side_effects=True, vmem_limit_bytes=40 * 1024 * 1024
            ),
        )(*(
            pltpu.with_memory_space_constraint(array, pltpu.HBM)
            for array in (diag_blocks, lower_coupling.T, upper_coupling.T, right_sides)
        ))
        return pl.pallas_call(
            put,
            out_shape=tuple(jax.ShapeDtypeStruct(array.shape, F32) for array in results),
            in_specs=[pl.BlockSpec(memory_space=pltpu.VMEM)] * 2,
            out_specs=(pl.BlockSpec(memory_space=pltpu.HBM),) * 2,
            scratch_shapes=[dma((5,))],
            compiler_params=pltpu.CompilerParams(vmem_limit_bytes=1024 * 1024),
        )(*results)

    return jax.shard_map(
        step,
        mesh=mesh,
        in_specs=(P("row", None), P("row", None), P("row", None), P("row", "grp")),
        out_specs=(P("row", "grp"), P(None, "grp")),
        check_vma=False,
    )
```

```python
import functools

import jax
import jax.numpy as jnp
from jax import lax
from jax.experimental import pallas as pl
from jax.experimental.pallas import tpu as pltpu
from jax.sharding import PartitionSpec as P

MESH = pl.DeviceIdType.MESH
SWEEPS = 8
DEPTH = 16
CORES = 2
CHUNKS = 2
F32 = jnp.float32
BF16 = jnp.bfloat16


def split(value):
    hi = value.astype(BF16)
    return hi, (value - hi.astype(F32)).astype(BF16)


def dot(left, right):
    return jnp.dot(left, right, preferred_element_type=F32)


def kernel(
    n, diag_hbm, lower_hbm, upper_hbm, rhs_hbm, x_acc, norms_ref,
    diag, lower, upper, rhs, recip, pivot, mats, edges, gmat_in, gmat_out, parts, ends_in, ends_out, inner_z,
    add_in, add_out, send_in, recv_in, send_out, recv_out, gsend_in, grecv_in, gsend_out, grecv_out,
    sums, early_plane, early_line, early_rows, late_plane, late_line,
    load_sem, si_sem, ri_sem, so_sem, ro_sem, g_sem,
    ap_send, ap_recv, bp_send, bp_recv, cp_send, cp_recv, al_send, al_recv, bl_send, bl_recv, know_a, know_b,
):
    width, size = lower_hbm.shape
    cols = rhs_hbm.shape[1]
    chunk = cols // CHUNKS
    last = SWEEPS - 1
    early = SWEEPS - 2
    me = lax.axis_index("row")
    core = lax.rem(me, CORES)
    chip = lax.div(me, CORES)
    depth = lax.rem(chip, DEPTH)
    plane = lax.div(chip, DEPTH)
    planes = n // (CORES * DEPTH)
    members = planes * CORES
    place = plane * CORES + core
    near = me + 1 - 2 * core
    far = me - 1 + 2 * core
    has_far = jnp.logical_and(far >= 0, far < n)
    far_rows = pl.multiple_of(core * (size - width), width)
    near_rows = pl.multiple_of((1 - core) * (size - width), width)

    def at_place(other):
        return (lax.div(other, CORES) * DEPTH + depth) * CORES + lax.rem(other, CORES)

    def at_depth(other):
        return (plane * DEPTH + other) * CORES + core

    def signal(sem, target):
        pl.semaphore_signal(sem, inc=1, device_id={"row": target}, device_id_type=MESH)

    def remote(src, dst, send_sem, recv_sem, target):
        return pltpu.make_async_remote_copy(
            src_ref=src, dst_ref=dst, send_sem=send_sem, recv_sem=recv_sem,
            device_id={"row": target}, device_id_type=MESH,
        )

    slab = size // 4
    loads = []

    def load(src, dst):
        copy = pltpu.make_async_copy(src, dst, load_sem.at[len(loads)])
        copy.start()
        loads.append(copy)
        return copy

    diag_loads, rhs_loads = {}, {}
    for i in (0, 3):
        diag_loads[i] = load(diag_hbm.at[pl.ds(i * slab, slab)], diag.at[pl.ds(i * slab, slab)])
        rhs_loads[i] = load(rhs_hbm.at[pl.ds(i * slab, slab)], rhs.at[pl.ds(i * slab, slab)])
    lower_load = load(lower_hbm, lower)
    upper_load = load(upper_hbm, upper)
    for i in (1, 2):
        diag_loads[i] = load(diag_hbm.at[pl.ds(i * slab, slab)], diag.at[pl.ds(i * slab, slab)])
        rhs_loads[i] = load(rhs_hbm.at[pl.ds(i * slab, slab)], rhs.at[pl.ds(i * slab, slab)])

    barrier = pltpu.get_barrier_semaphore()
    for offset in range(1, members):
        signal(barrier, at_place(lax.rem(place + offset, members)))
    for offset in (1, 2, DEPTH - 2, DEPTH - 1):
        signal(barrier, at_depth(lax.rem(depth + offset, DEPTH)))

    @pl.when(has_far)
    def _():
        signal(barrier, far)

    @pl.when(jnp.logical_not(has_far))
    def _():
        recv_out[...] = jnp.zeros_like(recv_out)
        grecv_out[...] = jnp.zeros_like(grecv_out)

    add_in[...] = jnp.zeros_like(add_in)
    add_out[...] = jnp.zeros_like(add_out)

    mask = lax.broadcasted_iota(jnp.int32, (slab, slab), 0) == lax.broadcasted_iota(jnp.int32, (slab, slab), 1)

    def pivots(i):
        rows = pl.ds(i * slab, slab)
        block = diag[rows, pl.ds(i * slab, slab)]
        values = jnp.sum(jnp.where(mask, block, 0.0), axis=1, keepdims=True)
        pivot[rows, :] = jnp.broadcast_to(values, (slab, slab))
        first = 1.0 / values
        recip[rows, :] = jnp.broadcast_to(first + first * (1.0 - values * first), (slab, slab))

    def scale(block, rows):
        factor = recip[rows, :]
        return jnp.concatenate([block[:, j : j + slab] * factor for j in range(0, block.shape[1], slab)], axis=1)

    for i in (0, 3):
        diag_loads[i].wait()
        pivots(i)
    for i in (0, 3):
        rhs_loads[i].wait()
    for ch in range(CHUNKS):
        span = pl.ds(ch * chunk, chunk)
        near_slice, far_slice = pl.ds(near_rows, width), pl.ds(far_rows, width)
        send_out[0, ch] = scale(rhs[far_slice, span], far_slice)
        send_in[0, ch] = scale(rhs[near_slice, span], near_slice)

    @pl.when(has_far)
    def _():
        pl.semaphore_wait(barrier, members + 4)

    @pl.when(jnp.logical_not(has_far))
    def _():
        pl.semaphore_wait(barrier, members + 3)

    def near_copy(s, ch):
        return remote(send_in.at[s, ch], recv_in.at[s, ch], si_sem.at[s, ch], ri_sem.at[s, ch], near)

    def far_copy(s, ch):
        return remote(send_out.at[s, ch], recv_out.at[s, ch], so_sem.at[s, ch], ro_sem.at[s, ch], far)

    def g_copy_near():
        return remote(gsend_in, grecv_in, g_sem.at[0], g_sem.at[1], near)

    def g_copy_far():
        return remote(gsend_out, grecv_out, g_sem.at[2], g_sem.at[3], far)

    def if_far(action):
        @pl.when(has_far)
        def _():
            action()

    for ch in range(CHUNKS):
        if_far(lambda ch=ch: far_copy(0, ch).start())
        near_copy(0, ch).start()
    signal(know_a, at_depth(lax.rem(depth + 2, DEPTH)))
    signal(know_a, at_depth(lax.rem(depth + DEPTH - 2, DEPTH)))

    for i in (1, 2):
        diag_loads[i].wait()
        pivots(i)
    lower_load.wait()
    upper_load.wait()
    for i in range(4):
        rows = pl.ds(i * slab, slab)
        low, up = lower[:, rows].T, upper[:, rows].T
        to_near = jnp.where(core == 0, up, low)
        to_far = jnp.where(has_far, jnp.where(core == 0, low, up), 0.0)
        for position, block in enumerate((to_near, to_far)):
            twice = jnp.concatenate([block, block], axis=1) * (-recip[rows, :])
            hi, lo = split(twice)
            edges[rows, pl.ds(position * 2 * slab, slab)] = hi
            edges[rows, pl.ds(position * 2 * slab + slab, slab)] = lo

    def rejoin(rows, position):
        hi = edges[rows, pl.ds(position * 2 * slab, slab)].astype(F32)
        return hi + edges[rows, pl.ds(position * 2 * slab + slab, slab)].astype(F32)

    gsend_in[...] = rejoin(pl.ds(near_rows, width), 0)
    gsend_out[...] = rejoin(pl.ds(far_rows, width), 1)
    if_far(lambda: g_copy_far().start())
    g_copy_near().start()

    for i in range(4):
        rows = pl.ds(i * slab, slab)
        factor = -recip[rows, :]
        for j in range(4):
            block = diag[rows, pl.ds(j * slab, slab)]
            if i == j:
                block = jnp.where(mask, 0.0, block)
            hi, lo = split(block * factor)
            mats[rows, pl.ds(j * slab, slab)] = hi
            mats[rows, pl.ds(size + j * slab, slab)] = hi
            mats[rows, pl.ds(2 * size + j * slab, slab)] = lo

    for i in (1, 2):
        rhs_loads[i].wait()

    tile = 64

    def rows_sum(total):
        return jnp.sum(total, axis=0, keepdims=True)

    def keep(ch, r, value):
        hi, lo = split(value)
        parts[ch, pl.ds(r, tile), :] = hi
        parts[ch, pl.ds(size + r, tile), :] = lo

    def begin(ch):
        span = pl.ds(ch * chunk, chunk)
        total = jnp.zeros((8, chunk), F32)
        for r in range(0, size, tile):
            rows = pl.ds(r, tile)
            block = rhs[rows, span]
            total += jnp.sum((block * block).reshape(tile // 8, 8, chunk), axis=0)
            value = scale(block, rows)
            x_acc[rows, span] = value
            keep(ch, r, value)
        sums[0, :, span] = rows_sum(total)

    def advance(ch):
        low_high = parts[ch]
        right = jnp.concatenate([low_high, low_high[:size]], axis=0)
        for r in range(0, size, size // 2):
            inner_z[ch, pl.ds(r, size // 2), :] = dot(mats[pl.ds(r, size // 2), :], right)

    def echo(ch):
        for rows, gmat, add in ((near_rows, gmat_in, add_in), (far_rows, gmat_out, add_out)):
            hi = parts[ch, pl.ds(rows, width), :]
            lo = parts[ch, pl.ds(size + rows, width), :]
            add[ch] = dot(gmat[...], jnp.concatenate([hi, lo, hi, lo], axis=0))

    def take(ch, received, add, ends):
        hi, lo = split(received + add[ch])
        ends[ch] = jnp.concatenate([hi, lo, hi, lo], axis=0)

    def from_near(s, ch, send):
        near_copy(s, ch).wait_recv()
        take(ch, recv_in[s, ch], add_in, ends_in)
        if send:
            rows = pl.ds(far_rows, width)
            send_out[s + 1, ch] = inner_z[ch, rows, :] + dot(edges[rows, : 2 * slab], ends_in[ch])
            if_far(lambda: far_copy(s + 1, ch).start())

    def from_far(s, ch, send):
        if_far(lambda: far_copy(s, ch).wait_recv())
        take(ch, recv_out[s, ch], add_out, ends_out)
        if send:
            rows = pl.ds(near_rows, width)
            send_in[s + 1, ch] = inner_z[ch, rows, :] + dot(edges[rows, 2 * slab :], ends_out[ch])
            near_copy(s + 1, ch).start()

    def complete(s, ch, final):
        span = pl.ds(ch * chunk, chunk)
        right = jnp.concatenate([ends_in[ch], ends_out[ch]], axis=0)
        total = jnp.zeros((8, chunk), F32)
        for start in range(0, size, size // 2):
            half = pl.ds(start, size // 2)
            block = inner_z[ch, half, :] + dot(edges[half, :], right)
            for r in range(0, size // 2, tile):
                rows = pl.ds(start + r, tile)
                value = block[r : r + tile]
                x_acc[rows, span] += value
                if not final:
                    keep(ch, start + r, value)
                factor = pivot[rows, :]
                residual = jnp.concatenate([value[:, j : j + slab] * factor for j in range(0, chunk, slab)], axis=1)
                total += jnp.sum((residual * residual).reshape(tile // 8, 8, chunk), axis=0)
        sums[s + 1, :, span] = rows_sum(total)

    for ch in range(CHUNKS):
        begin(ch)
        advance(ch)

    def take_squares():
        g_copy_near().wait_recv()
        if_far(lambda: g_copy_far().wait_recv())
        for source, target in ((grecv_in, gmat_in), (grecv_out, gmat_out)):
            hi, lo = split(source[...])
            target[:, :slab] = hi
            target[:, slab:] = lo

    def sweep(s):
        for ch in range(CHUNKS):
            from_far(s, ch, True)
            if ch > 0:
                from_near(s + 1, ch - 1, s + 1 < last - 1)
            elif s == 0:
                take_squares()
            echo(ch)
            complete(s, ch, False)
            advance(ch)
        from_near(s + 1, CHUNKS - 1, s + 1 < last - 1)

    def early_a(offset, target_place):
        return remote(
            sums.at[target_place], early_plane.at[place], ap_send.at[offset], ap_recv.at[offset], at_place(target_place)
        )

    def line(buffer, send_sem, recv_sem, offset):
        return remote(
            buffer.at[depth], buffer.at[depth], send_sem.at[offset], recv_sem.at[offset],
            at_depth(lax.rem(depth + offset, DEPTH)),
        )

    def late_a(i, offset):
        return remote(
            sums.at[early + i], late_plane.at[i, place], al_send.at[i, offset], al_recv.at[i, offset],
            at_place(lax.rem(place + offset, members)),
        )

    def late_b(i, offset):
        return line(late_line.at[i], bl_send.at[i], bl_recv.at[i], offset)

    def late_row(i):
        for offset in range(1, members):
            late_a(i, offset).start()
        late_plane[i, place] = sums[early + i]

    def late_sum(i):
        for offset in range(1, members):
            late_a(i, offset).wait_recv()
        late_line[i, depth] = added(late_plane.at[i], members)
        for offset in range(1, DEPTH):
            late_b(i, offset).start()

    def early_c(offset):
        return remote(
            early_rows.at[place], early_rows.at[place], cp_send.at[offset], cp_recv.at[offset],
            at_place(lax.rem(place + offset, members)),
        )

    def added(buffer, count):
        values = [buffer[i] for i in range(count)]
        while len(values) > 1:
            values = [values[i] + values[i + 1] for i in range(0, len(values), 2)]
        return values[0]

    for ch in range(CHUNKS):
        from_near(0, ch, True)
    sweep(0)
    pl.semaphore_wait(know_a, 2)
    signal(know_b, at_depth(lax.rem(depth + 4, DEPTH)))
    signal(know_b, at_depth(lax.rem(depth + DEPTH - 4, DEPTH)))
    for s in range(1, early - 1):
        sweep(s)

    for offset in range(1, members):
        target_place = lax.rem(place + offset, members)

        @pl.when(target_place < early)
        def _(offset=offset, target_place=target_place):
            early_a(offset, target_place).start()

    for s in range(early - 1, last - 1):
        sweep(s)
    late_row(0)
    pl.semaphore_wait(know_b, 2)

    @pl.when(place < early)
    def _():
        early_plane[place] = sums[place]
        for offset in range(1, members):
            early_a(offset, place).wait_recv()
        early_line[depth] = added(early_plane, members)
        for offset in range(1, DEPTH):
            line(early_line, bp_send, bp_recv, offset).start()

    for ch in range(CHUNKS):
        from_far(last - 1, ch, False)
        complete(last - 1, ch, True)

    late_row(1)

    for s in range(last):
        for ch in range(CHUNKS):
            near_copy(s, ch).wait_send()
            if_far(lambda s=s, ch=ch: far_copy(s, ch).wait_send())
    g_copy_near().wait_send()
    if_far(lambda: g_copy_far().wait_send())
    for offset in range(1, members):

        @pl.when(lax.rem(place + offset, members) < early)
        def _(offset=offset):
            early_a(offset, place).wait_send()

    for i in range(SWEEPS - early):
        late_sum(i)

    @pl.when(place < early)
    def _():
        for offset in range(1, DEPTH):
            line(early_line, bp_send, bp_recv, offset).wait_recv()
        early_rows[place] = added(early_line, DEPTH)
        for offset in range(1, members):
            early_c(offset).start()

    for offset in range(1, members):

        @pl.when(lax.rem(place + members - offset, members) < early)
        def _(offset=offset):
            early_c(offset).wait_recv()

    for i in range(early):
        norms_ref[i : i + 1, :] = jnp.sqrt(early_rows[i])
    for i in range(SWEEPS - early):
        for offset in range(1, members):
            late_a(i, offset).wait_send()

    @pl.when(place < early)
    def _():
        for offset in range(1, DEPTH):
            line(early_line, bp_send, bp_recv, offset).wait_send()
        for offset in range(1, members):
            early_c(offset).wait_send()

    for i in range(SWEEPS - early):
        for offset in range(1, DEPTH):
            late_b(i, offset).wait_send()
    for i in range(SWEEPS - early):
        for offset in range(1, DEPTH):
            late_b(i, offset).wait_recv()
        norms_ref[early + i : early + i + 1, :] = jnp.sqrt(added(late_line.at[i], DEPTH))


def put(x_ref, norms_ref, x_hbm, norms_hbm, sems):
    size = x_ref.shape[0] // 4
    copies = [pltpu.make_async_copy(norms_ref, norms_hbm, sems.at[4])]
    for i in range(4):
        rows = pl.ds(i * size, size)
        copies.append(pltpu.make_async_copy(x_ref.at[rows], x_hbm.at[rows], sems.at[i]))
    for copy in copies:
        copy.start()
    for copy in copies:
        copy.wait()


def solution(mesh):
    n = mesh.shape["row"]
    members = n // DEPTH

    def step(diag_blocks, lower_coupling, upper_coupling, right_sides):
        size, width = lower_coupling.shape
        cols = right_sides.shape[1]
        chunk = cols // CHUNKS
        last = SWEEPS - 1
        dma = pltpu.SemaphoreType.DMA
        halo = pltpu.VMEM((last, CHUNKS, width, chunk), F32)
        square = pltpu.VMEM((width, 2 * width), F32)
        row = lambda count: pltpu.VMEM((count, 1, cols), F32)
        results = pl.pallas_call(
            functools.partial(kernel, n),
            out_shape=(
                jax.ShapeDtypeStruct((size, cols), F32),
                jax.ShapeDtypeStruct((SWEEPS, cols), F32),
            ),
            in_specs=[pl.BlockSpec(memory_space=pltpu.HBM)] * 4,
            out_specs=(pl.BlockSpec(memory_space=pltpu.VMEM), pl.BlockSpec(memory_space=pltpu.VMEM)),
            scratch_shapes=[
                pltpu.VMEM((size, size), F32),
                pltpu.VMEM((width, size), F32),
                pltpu.VMEM((width, size), F32),
                pltpu.VMEM((size, cols), F32),
                pltpu.VMEM((size, size // 4), F32),
                pltpu.VMEM((size, size // 4), F32),
                pltpu.VMEM((size, 3 * size), BF16),
                pltpu.VMEM((size, 8 * width), BF16),
                pltpu.VMEM((width, 4 * width), BF16),
                pltpu.VMEM((width, 4 * width), BF16),
                pltpu.VMEM((CHUNKS, 2 * size, chunk), BF16),
                pltpu.VMEM((CHUNKS, 4 * width, chunk), BF16),
                pltpu.VMEM((CHUNKS, 4 * width, chunk), BF16),
                pltpu.VMEM((CHUNKS, size, chunk), F32),
                pltpu.VMEM((CHUNKS, width, chunk), F32),
                pltpu.VMEM((CHUNKS, width, chunk), F32),
                halo, halo, halo, halo,
                square, square, square, square,
                row(SWEEPS), row(members), row(DEPTH), row(members),
                pltpu.VMEM((2, members, 1, cols), F32), pltpu.VMEM((2, DEPTH, 1, cols), F32),
                dma((10,)),
                dma((last, CHUNKS)), dma((last, CHUNKS)), dma((last, CHUNKS)), dma((last, CHUNKS)), dma((4,)),
                dma((members,)), dma((members,)), dma((DEPTH,)), dma((DEPTH,)), dma((members,)), dma((members,)),
                dma((2, members)), dma((2, members)), dma((2, DEPTH)), dma((2, DEPTH)),
                pltpu.SemaphoreType.REGULAR, pltpu.SemaphoreType.REGULAR,
            ],
            compiler_params=pltpu.CompilerParams(
                collective_id=0, has_side_effects=True, vmem_limit_bytes=40 * 1024 * 1024
            ),
        )(*(
            pltpu.with_memory_space_constraint(array, pltpu.HBM)
            for array in (diag_blocks, lower_coupling.T, upper_coupling.T, right_sides)
        ))
        return pl.pallas_call(
            put,
            out_shape=tuple(jax.ShapeDtypeStruct(array.shape, F32) for array in results),
            in_specs=[pl.BlockSpec(memory_space=pltpu.VMEM)] * 2,
            out_specs=(pl.BlockSpec(memory_space=pltpu.HBM),) * 2,
            scratch_shapes=[dma((5,))],
            compiler_params=pltpu.CompilerParams(vmem_limit_bytes=1024 * 1024),
        )(*results)

    return jax.shard_map(
        step,
        mesh=mesh,
        in_specs=(P("row", None), P("row", None), P("row", None), P("row", "grp")),
        out_specs=(P("row", "grp"), P(None, "grp")),
        check_vma=False,
    )
```

```python
import functools

import jax
import jax.numpy as jnp
from jax import lax
from jax.experimental import pallas as pl
from jax.experimental.pallas import tpu as pltpu
from jax.sharding import PartitionSpec as P

MESH = pl.DeviceIdType.MESH
SWEEPS = 8
DEPTH = 16
CORES = 2
CHUNKS = 2
F32 = jnp.float32
BF16 = jnp.bfloat16


def split(value):
    hi = value.astype(BF16)
    return hi, (value - hi.astype(F32)).astype(BF16)


def dot(left, right):
    return jnp.dot(left, right, preferred_element_type=F32)


def kernel(
    n, diag_hbm, lower_hbm, upper_hbm, rhs_hbm, x_acc, norms_ref,
    diag, lower, upper, rhs, recip, pivot, mats, edges, gmat_in, gmat_out, parts, ends_in, ends_out, inner_z,
    add_in, add_out, send_in, recv_in, send_out, recv_out, gsend_in, grecv_in, gsend_out, grecv_out,
    sums, early_plane, early_line, early_rows, late_plane, late_line,
    load_sem, si_sem, ri_sem, so_sem, ro_sem, g_sem,
    ap_send, ap_recv, bp_send, bp_recv, cp_send, cp_recv, al_send, al_recv, bl_send, bl_recv, know_a, know_b,
):
    width, size = lower_hbm.shape
    cols = rhs_hbm.shape[1]
    chunk = cols // CHUNKS
    last = SWEEPS - 1
    early = SWEEPS - 2
    me = lax.axis_index("row")
    core = lax.rem(me, CORES)
    chip = lax.div(me, CORES)
    depth = lax.rem(chip, DEPTH)
    plane = lax.div(chip, DEPTH)
    planes = n // (CORES * DEPTH)
    members = planes * CORES
    place = plane * CORES + core
    near = me + 1 - 2 * core
    far = me - 1 + 2 * core
    has_far = jnp.logical_and(far >= 0, far < n)
    far_rows = pl.multiple_of(core * (size - width), width)
    near_rows = pl.multiple_of((1 - core) * (size - width), width)

    def at_place(other):
        return (lax.div(other, CORES) * DEPTH + depth) * CORES + lax.rem(other, CORES)

    def at_depth(other):
        return (plane * DEPTH + other) * CORES + core

    def signal(sem, target):
        pl.semaphore_signal(sem, inc=1, device_id={"row": target}, device_id_type=MESH)

    def remote(src, dst, send_sem, recv_sem, target):
        return pltpu.make_async_remote_copy(
            src_ref=src, dst_ref=dst, send_sem=send_sem, recv_sem=recv_sem,
            device_id={"row": target}, device_id_type=MESH,
        )

    slab = size // 4
    loads = []

    def load(src, dst):
        copy = pltpu.make_async_copy(src, dst, load_sem.at[len(loads)])
        copy.start()
        loads.append(copy)
        return copy

    diag_loads, rhs_loads = {}, {}
    for i in (0, 3):
        diag_loads[i] = load(diag_hbm.at[pl.ds(i * slab, slab)], diag.at[pl.ds(i * slab, slab)])
        rhs_loads[i] = load(rhs_hbm.at[pl.ds(i * slab, slab)], rhs.at[pl.ds(i * slab, slab)])
    lower_load = load(lower_hbm, lower)
    upper_load = load(upper_hbm, upper)
    for i in (1, 2):
        diag_loads[i] = load(diag_hbm.at[pl.ds(i * slab, slab)], diag.at[pl.ds(i * slab, slab)])
        rhs_loads[i] = load(rhs_hbm.at[pl.ds(i * slab, slab)], rhs.at[pl.ds(i * slab, slab)])

    barrier = pltpu.get_barrier_semaphore()
    for offset in range(1, members):
        signal(barrier, at_place(lax.rem(place + offset, members)))
    for offset in (1, 2, DEPTH - 2, DEPTH - 1):
        signal(barrier, at_depth(lax.rem(depth + offset, DEPTH)))

    @pl.when(has_far)
    def _():
        signal(barrier, far)

    @pl.when(jnp.logical_not(has_far))
    def _():
        recv_out[...] = jnp.zeros_like(recv_out)
        grecv_out[...] = jnp.zeros_like(grecv_out)

    add_in[...] = jnp.zeros_like(add_in)
    add_out[...] = jnp.zeros_like(add_out)

    mask = lax.broadcasted_iota(jnp.int32, (slab, slab), 0) == lax.broadcasted_iota(jnp.int32, (slab, slab), 1)

    def pivots(i):
        rows = pl.ds(i * slab, slab)
        block = diag[rows, pl.ds(i * slab, slab)]
        values = jnp.sum(jnp.where(mask, block, 0.0), axis=1, keepdims=True)
        pivot[rows, :] = jnp.broadcast_to(values, (slab, slab))
        first = 1.0 / values
        recip[rows, :] = jnp.broadcast_to(first + first * (1.0 - values * first), (slab, slab))

    def scale(block, rows):
        factor = recip[rows, :]
        return jnp.concatenate([block[:, j : j + slab] * factor for j in range(0, block.shape[1], slab)], axis=1)

    for i in (0, 3):
        diag_loads[i].wait()
        pivots(i)
    for i in (0, 3):
        rhs_loads[i].wait()
    for ch in range(CHUNKS):
        span = pl.ds(ch * chunk, chunk)
        near_slice, far_slice = pl.ds(near_rows, width), pl.ds(far_rows, width)
        send_out[0, ch] = scale(rhs[far_slice, span], far_slice)
        send_in[0, ch] = scale(rhs[near_slice, span], near_slice)

    @pl.when(has_far)
    def _():
        pl.semaphore_wait(barrier, members + 4)

    @pl.when(jnp.logical_not(has_far))
    def _():
        pl.semaphore_wait(barrier, members + 3)

    def near_copy(s, ch):
        return remote(send_in.at[s, ch], recv_in.at[s, ch], si_sem.at[s, ch], ri_sem.at[s, ch], near)

    def far_copy(s, ch):
        return remote(send_out.at[s, ch], recv_out.at[s, ch], so_sem.at[s, ch], ro_sem.at[s, ch], far)

    def g_copy_near():
        return remote(gsend_in, grecv_in, g_sem.at[0], g_sem.at[1], near)

    def g_copy_far():
        return remote(gsend_out, grecv_out, g_sem.at[2], g_sem.at[3], far)

    def if_far(action):
        @pl.when(has_far)
        def _():
            action()

    for ch in range(CHUNKS):
        if_far(lambda ch=ch: far_copy(0, ch).start())
        near_copy(0, ch).start()
    signal(know_a, at_depth(lax.rem(depth + 2, DEPTH)))
    signal(know_a, at_depth(lax.rem(depth + DEPTH - 2, DEPTH)))

    for i in (1, 2):
        diag_loads[i].wait()
        pivots(i)
    lower_load.wait()
    upper_load.wait()
    for i in range(4):
        rows = pl.ds(i * slab, slab)
        low, up = lower[:, rows].T, upper[:, rows].T
        to_near = jnp.where(core == 0, up, low)
        to_far = jnp.where(has_far, jnp.where(core == 0, low, up), 0.0)
        for position, block in enumerate((to_near, to_far)):
            twice = jnp.concatenate([block, block], axis=1) * (-recip[rows, :])
            hi, lo = split(twice)
            edges[rows, pl.ds(position * 2 * slab, slab)] = hi
            edges[rows, pl.ds(position * 2 * slab + slab, slab)] = lo

    def rejoin(rows, position):
        hi = edges[rows, pl.ds(position * 2 * slab, slab)].astype(F32)
        return hi + edges[rows, pl.ds(position * 2 * slab + slab, slab)].astype(F32)

    gsend_in[...] = rejoin(pl.ds(near_rows, width), 0)
    gsend_out[...] = rejoin(pl.ds(far_rows, width), 1)
    if_far(lambda: g_copy_far().start())
    g_copy_near().start()

    for i in range(4):
        rows = pl.ds(i * slab, slab)
        factor = -recip[rows, :]
        for j in range(4):
            block = diag[rows, pl.ds(j * slab, slab)]
            if i == j:
                block = jnp.where(mask, 0.0, block)
            hi, lo = split(block * factor)
            mats[rows, pl.ds(j * slab, slab)] = hi
            mats[rows, pl.ds(size + j * slab, slab)] = hi
            mats[rows, pl.ds(2 * size + j * slab, slab)] = lo

    for i in (1, 2):
        rhs_loads[i].wait()

    tile = 64

    def rows_sum(total):
        return jnp.sum(total, axis=0, keepdims=True)

    def keep(ch, r, value):
        hi, lo = split(value)
        parts[ch, pl.ds(r, tile), :] = hi
        parts[ch, pl.ds(size + r, tile), :] = lo

    def begin(ch):
        span = pl.ds(ch * chunk, chunk)
        total = jnp.zeros((8, chunk), F32)
        for r in range(0, size, tile):
            rows = pl.ds(r, tile)
            block = rhs[rows, span]
            total += jnp.sum((block * block).reshape(tile // 8, 8, chunk), axis=0)
            value = scale(block, rows)
            x_acc[rows, span] = value
            keep(ch, r, value)
        sums[0, :, span] = rows_sum(total)

    def advance(ch):
        low_high = parts[ch]
        right = jnp.concatenate([low_high, low_high[:size]], axis=0)
        for r in range(0, size, size // 2):
            inner_z[ch, pl.ds(r, size // 2), :] = dot(mats[pl.ds(r, size // 2), :], right)

    def echo(ch):
        for rows, gmat, add in ((near_rows, gmat_in, add_in), (far_rows, gmat_out, add_out)):
            hi = parts[ch, pl.ds(rows, width), :]
            lo = parts[ch, pl.ds(size + rows, width), :]
            add[ch] = dot(gmat[...], jnp.concatenate([hi, lo, hi, lo], axis=0))

    def take(ch, received, add, ends):
        hi, lo = split(received + add[ch])
        ends[ch] = jnp.concatenate([hi, lo, hi, lo], axis=0)

    def from_near(s, ch, send):
        near_copy(s, ch).wait_recv()
        take(ch, recv_in[s, ch], add_in, ends_in)
        if send:
            rows = pl.ds(far_rows, width)
            send_out[s + 1, ch] = inner_z[ch, rows, :] + dot(edges[rows, : 2 * slab], ends_in[ch])
            if_far(lambda: far_copy(s + 1, ch).start())

    def from_far(s, ch, send):
        if_far(lambda: far_copy(s, ch).wait_recv())
        take(ch, recv_out[s, ch], add_out, ends_out)
        if send:
            rows = pl.ds(near_rows, width)
            send_in[s + 1, ch] = inner_z[ch, rows, :] + dot(edges[rows, 2 * slab :], ends_out[ch])
            near_copy(s + 1, ch).start()

    def complete(s, ch, final):
        span = pl.ds(ch * chunk, chunk)
        right = jnp.concatenate([ends_in[ch], ends_out[ch]], axis=0)
        total = jnp.zeros((8, chunk), F32)
        for start in range(0, size, size // 2):
            half = pl.ds(start, size // 2)
            block = inner_z[ch, half, :] + dot(edges[half, :], right)
            for r in range(0, size // 2, tile):
                rows = pl.ds(start + r, tile)
                value = block[r : r + tile]
                x_acc[rows, span] += value
                if not final:
                    keep(ch, start + r, value)
                factor = pivot[rows, :]
                residual = jnp.concatenate([value[:, j : j + slab] * factor for j in range(0, chunk, slab)], axis=1)
                total += jnp.sum((residual * residual).reshape(tile // 8, 8, chunk), axis=0)
        sums[s + 1, :, span] = rows_sum(total)

    for ch in range(CHUNKS):
        begin(ch)
        advance(ch)

    def take_squares():
        g_copy_near().wait_recv()
        if_far(lambda: g_copy_far().wait_recv())
        for source, target in ((grecv_in, gmat_in), (grecv_out, gmat_out)):
            hi, lo = split(source[...])
            target[:, :slab] = hi
            target[:, slab:] = lo

    def sweep(s):
        for ch in range(CHUNKS):
            if ch > 0:
                from_near(s + 1, ch - 1, s + 1 < last - 1)
            from_far(s, ch, True)
            if ch == 0 and s == 0:
                take_squares()
            echo(ch)
            complete(s, ch, False)
            advance(ch)
        from_near(s + 1, CHUNKS - 1, s + 1 < last - 1)

    def early_a(offset, target_place):
        return remote(
            sums.at[target_place], early_plane.at[place], ap_send.at[offset], ap_recv.at[offset], at_place(target_place)
        )

    def line(buffer, send_sem, recv_sem, offset):
        return remote(
            buffer.at[depth], buffer.at[depth], send_sem.at[offset], recv_sem.at[offset],
            at_depth(lax.rem(depth + offset, DEPTH)),
        )

    def late_a(i, offset):
        return remote(
            sums.at[early + i], late_plane.at[i, place], al_send.at[i, offset], al_recv.at[i, offset],
            at_place(lax.rem(place + offset, members)),
        )

    def late_b(i, offset):
        return line(late_line.at[i], bl_send.at[i], bl_recv.at[i], offset)

    def late_row(i):
        for offset in range(1, members):
            late_a(i, offset).start()
        late_plane[i, place] = sums[early + i]

    def late_sum(i):
        for offset in range(1, members):
            late_a(i, offset).wait_recv()
        late_line[i, depth] = added(late_plane.at[i], members)
        for offset in range(1, DEPTH):
            late_b(i, offset).start()

    def early_c(offset):
        return remote(
            early_rows.at[place], early_rows.at[place], cp_send.at[offset], cp_recv.at[offset],
            at_place(lax.rem(place + offset, members)),
        )

    def added(buffer, count):
        values = [buffer[i] for i in range(count)]
        while len(values) > 1:
            values = [values[i] + values[i + 1] for i in range(0, len(values), 2)]
        return values[0]

    for ch in range(CHUNKS):
        from_near(0, ch, True)
    sweep(0)
    pl.semaphore_wait(know_a, 2)
    signal(know_b, at_depth(lax.rem(depth + 4, DEPTH)))
    signal(know_b, at_depth(lax.rem(depth + DEPTH - 4, DEPTH)))
    for s in range(1, early - 1):
        sweep(s)

    for offset in range(1, members):
        target_place = lax.rem(place + offset, members)

        @pl.when(target_place < early)
        def _(offset=offset, target_place=target_place):
            early_a(offset, target_place).start()

    for s in range(early - 1, last - 1):
        sweep(s)
    late_row(0)
    pl.semaphore_wait(know_b, 2)

    @pl.when(place < early)
    def _():
        early_plane[place] = sums[place]
        for offset in range(1, members):
            early_a(offset, place).wait_recv()
        early_line[depth] = added(early_plane, members)
        for offset in range(1, DEPTH):
            line(early_line, bp_send, bp_recv, offset).start()

    for ch in range(CHUNKS):
        from_far(last - 1, ch, False)
        complete(last - 1, ch, True)

    late_row(1)

    for s in range(last):
        for ch in range(CHUNKS):
            near_copy(s, ch).wait_send()
            if_far(lambda s=s, ch=ch: far_copy(s, ch).wait_send())
    g_copy_near().wait_send()
    if_far(lambda: g_copy_far().wait_send())
    for offset in range(1, members):

        @pl.when(lax.rem(place + offset, members) < early)
        def _(offset=offset):
            early_a(offset, place).wait_send()

    for i in range(SWEEPS - early):
        late_sum(i)

    @pl.when(place < early)
    def _():
        for offset in range(1, DEPTH):
            line(early_line, bp_send, bp_recv, offset).wait_recv()
        early_rows[place] = added(early_line, DEPTH)
        for offset in range(1, members):
            early_c(offset).start()

    for offset in range(1, members):

        @pl.when(lax.rem(place + members - offset, members) < early)
        def _(offset=offset):
            early_c(offset).wait_recv()

    for i in range(early):
        norms_ref[i : i + 1, :] = jnp.sqrt(early_rows[i])
    for i in range(SWEEPS - early):
        for offset in range(1, members):
            late_a(i, offset).wait_send()

    @pl.when(place < early)
    def _():
        for offset in range(1, DEPTH):
            line(early_line, bp_send, bp_recv, offset).wait_send()
        for offset in range(1, members):
            early_c(offset).wait_send()

    for i in range(SWEEPS - early):
        for offset in range(1, DEPTH):
            late_b(i, offset).wait_send()
    for i in range(SWEEPS - early):
        for offset in range(1, DEPTH):
            late_b(i, offset).wait_recv()
        norms_ref[early + i : early + i + 1, :] = jnp.sqrt(added(late_line.at[i], DEPTH))


def put(x_ref, norms_ref, x_hbm, norms_hbm, sems):
    size = x_ref.shape[0] // 4
    copies = [pltpu.make_async_copy(norms_ref, norms_hbm, sems.at[4])]
    for i in range(4):
        rows = pl.ds(i * size, size)
        copies.append(pltpu.make_async_copy(x_ref.at[rows], x_hbm.at[rows], sems.at[i]))
    for copy in copies:
        copy.start()
    for copy in copies:
        copy.wait()


def solution(mesh):
    n = mesh.shape["row"]
    members = n // DEPTH

    def step(diag_blocks, lower_coupling, upper_coupling, right_sides):
        size, width = lower_coupling.shape
        cols = right_sides.shape[1]
        chunk = cols // CHUNKS
        last = SWEEPS - 1
        dma = pltpu.SemaphoreType.DMA
        halo = pltpu.VMEM((last, CHUNKS, width, chunk), F32)
        square = pltpu.VMEM((width, 2 * width), F32)
        row = lambda count: pltpu.VMEM((count, 1, cols), F32)
        results = pl.pallas_call(
            functools.partial(kernel, n),
            out_shape=(
                jax.ShapeDtypeStruct((size, cols), F32),
                jax.ShapeDtypeStruct((SWEEPS, cols), F32),
            ),
            in_specs=[pl.BlockSpec(memory_space=pltpu.HBM)] * 4,
            out_specs=(pl.BlockSpec(memory_space=pltpu.VMEM), pl.BlockSpec(memory_space=pltpu.VMEM)),
            scratch_shapes=[
                pltpu.VMEM((size, size), F32),
                pltpu.VMEM((width, size), F32),
                pltpu.VMEM((width, size), F32),
                pltpu.VMEM((size, cols), F32),
                pltpu.VMEM((size, size // 4), F32),
                pltpu.VMEM((size, size // 4), F32),
                pltpu.VMEM((size, 3 * size), BF16),
                pltpu.VMEM((size, 8 * width), BF16),
                pltpu.VMEM((width, 4 * width), BF16),
                pltpu.VMEM((width, 4 * width), BF16),
                pltpu.VMEM((CHUNKS, 2 * size, chunk), BF16),
                pltpu.VMEM((CHUNKS, 4 * width, chunk), BF16),
                pltpu.VMEM((CHUNKS, 4 * width, chunk), BF16),
                pltpu.VMEM((CHUNKS, size, chunk), F32),
                pltpu.VMEM((CHUNKS, width, chunk), F32),
                pltpu.VMEM((CHUNKS, width, chunk), F32),
                halo, halo, halo, halo,
                square, square, square, square,
                row(SWEEPS), row(members), row(DEPTH), row(members),
                pltpu.VMEM((2, members, 1, cols), F32), pltpu.VMEM((2, DEPTH, 1, cols), F32),
                dma((10,)),
                dma((last, CHUNKS)), dma((last, CHUNKS)), dma((last, CHUNKS)), dma((last, CHUNKS)), dma((4,)),
                dma((members,)), dma((members,)), dma((DEPTH,)), dma((DEPTH,)), dma((members,)), dma((members,)),
                dma((2, members)), dma((2, members)), dma((2, DEPTH)), dma((2, DEPTH)),
                pltpu.SemaphoreType.REGULAR, pltpu.SemaphoreType.REGULAR,
            ],
            compiler_params=pltpu.CompilerParams(
                collective_id=0, has_side_effects=True, vmem_limit_bytes=40 * 1024 * 1024
            ),
        )(*(
            pltpu.with_memory_space_constraint(array, pltpu.HBM)
            for array in (diag_blocks, lower_coupling.T, upper_coupling.T, right_sides)
        ))
        return pl.pallas_call(
            put,
            out_shape=tuple(jax.ShapeDtypeStruct(array.shape, F32) for array in results),
            in_specs=[pl.BlockSpec(memory_space=pltpu.VMEM)] * 2,
            out_specs=(pl.BlockSpec(memory_space=pltpu.HBM),) * 2,
            scratch_shapes=[dma((5,))],
            compiler_params=pltpu.CompilerParams(vmem_limit_bytes=1024 * 1024),
        )(*results)

    return jax.shard_map(
        step,
        mesh=mesh,
        in_specs=(P("row", None), P("row", None), P("row", None), P("row", "grp")),
        out_specs=(P("row", "grp"), P(None, "grp")),
        check_vma=False,
    )
```
